512 devices in a mesh: atoms: 64 (over x, y, core), chan: 8 (over z).
Axes of the slice: x: 4, y: 8, z: 8, core: 2. Of those that a mesh axis runs over, the one named last changes fastest.
Arguments:
- features: bfloat16 [128, 32768], P('chan', 'atoms'), may hold values from -6 to 6
- positions: float32 [3, 32768], P(None, 'atoms'), may hold values from 0 to 384
- block_counts: int32 [256], P('atoms'), may hold values from 64 to 128
- radial_w: float32 [8, 3, 128], P(None, None, 'chan'), may hold values from -2 to 2
- mix_w: bfloat16 [4, 128, 128], replicated, may hold values from -0.25 to 0.25
- read_w: float32 [128], P('chan'), may hold values from -0.5 to 0.5
- ghost_lists: int32 [64, 2, 2], P('atoms'), may hold values from 0 to 3, as said below
- tile_pairs: int32 [64, 24, 2], P('atoms'), may hold values from 0 to 7, as said below
- tile_count: int32 [64], P('atoms'), may hold values from 9 to 24, as said below
Outputs:
- updated: bfloat16 [128, 32768], P('chan', 'atoms')
- energies: float32 [32768], P('atoms')
- scale: float32 [], replicated
The draws below stay inside these ranges and needn't reach their ends.
Inputs may be any that keep to these rules, and one draw needn't show every extreme that they name: `ghost_lists`: row 0 of group g lists each of its even-numbered blocks once and row 1 each odd-numbered block once, in some order. `tile_pairs`: codes below 4 name the group's own block, codes 4 to 5 a slot of the previous group's ghost_lists row 1, higher codes a slot of the next group's row 0; no code points outside the first or last group. Tile t < 4 of each group is (t, t). Tiles from tile_count[g] on are (0, 0). `tile_count`: some group has 24 live tiles.
All inputs are finite; a program needn't handle non-finite values.
Results may differ from the reference program's by a relative error of at most 0.007.
Values may be sent and summed in bfloat16 or wider, within the bound.
A program may use at most 64 MiB of HBM per device.

```python
import math
import jax
import jax.numpy as jnp
from jax import lax

C = 128
NR = 8
BLK = 128
BLK_DEV = 4
GHOST = 2
TILES_DEV = 24
SHARDS = 64
BLOCKS = 256
ATOMS = 32768


pitch_across = 3.0


def draw_positions(key, part):
    atom = jnp.arange(ATOMS, dtype=jnp.int32)
    block = atom // BLK
    group = block // BLK_DEV
    local = block % BLK_DEV
    column = local // 2
    cells = jnp.stack([2 * group + local % 2, column // 2, column % 2]).astype(jnp.float32)
    jitter = jax.random.uniform(jax.random.fold_in(key, 3), (3, ATOMS), jnp.float32)
    pitch_side = math.sqrt(BLK * 4.0 / 3.0)
    pitches = jnp.array([pitch_across, pitch_side, pitch_side], jnp.float32)
    return (cells + jitter) * pitches[:, None]


def ghost_rows(key):
    subkeys = jax.random.split(jax.random.fold_in(key, 5), SHARDS * 2)
    orders = jax.vmap(lambda subkey: jax.random.permutation(subkey, GHOST))(subkeys).reshape(SHARDS, 2, GHOST)
    return (2 * orders + jnp.arange(2, dtype=jnp.int32)[None, :, None]).astype(jnp.int32)


def draw_ghost_lists(key, part):
    return ghost_rows(key)


def draw_tile_count(key, part):
    lowest = BLK_DEV + (TILES_DEV - BLK_DEV) // 4
    counts = jax.random.randint(jax.random.fold_in(key, 7), (SHARDS,), lowest, TILES_DEV + 1)
    fullest = jax.random.randint(jax.random.fold_in(key, 8), (), 0, SHARDS)
    return jnp.where(jnp.arange(SHARDS) == fullest, TILES_DEV, counts).astype(jnp.int32)


def draw_tile_pairs(key, part):
    counts = draw_tile_count(key, part)
    lists = ghost_rows(key)
    subkeys = jax.random.split(jax.random.fold_in(key, 9), SHARDS)
    slots = jnp.arange(GHOST, dtype=jnp.int32)

    def one_group(subkey, device, total):
        pieces = jax.random.split(subkey, 3)
        places = jnp.arange(TILES_DEV)
        receivers = jax.random.randint(pieces[0], (TILES_DEV,), 0, BLK_DEV)
        moves = jax.random.randint(pieces[1], (TILES_DEV, 3), -1, 2)
        forced = (places >= BLK_DEV) & (places < BLK_DEV + 4)
        side = (places - BLK_DEV) % 2
        forced_column = jax.random.randint(pieces[2], (TILES_DEV,), 0, GHOST)
        receivers = jnp.where(forced, 2 * forced_column + side, receivers)
        forced_moves = jnp.stack([2 * side - 1, jnp.zeros_like(side), jnp.zeros_like(side)], axis=-1)
        moves = jnp.where(forced[:, None], forced_moves, moves)
        column = receivers // 2
        cell_x = 2 * device + receivers % 2 + moves[:, 0]
        cell_y = column // 2 + moves[:, 1]
        cell_z = column % 2 + moves[:, 2]
        target_column = 2 * cell_y + cell_z
        valid = (cell_y >= 0) & (cell_z >= 0) & (cell_z <= 1) & (target_column < GHOST) & (cell_x >= 0) & (cell_x < 2 * SHARDS)
        target_group = jnp.where(valid, cell_x // 2, device)
        target_block = jnp.clip(2 * target_column + cell_x % 2, 0, BLK_DEV - 1)
        left_row = lists[jnp.maximum(device - 1, 0), 1]
        right_row = lists[jnp.minimum(device + 1, SHARDS - 1), 0]
        left_slot = jnp.sum(jnp.where(left_row[None, :] == target_block[:, None], slots[None, :], 0), axis=1)
        right_slot = jnp.sum(jnp.where(right_row[None, :] == target_block[:, None], slots[None, :], 0), axis=1)
        codes = jnp.where(target_group == device, target_block, jnp.where(target_group == device - 1, BLK_DEV + left_slot, BLK_DEV + GHOST + right_slot))
        codes = jnp.where(valid, codes, receivers)
        receivers = jnp.where(places < BLK_DEV, places, receivers)
        codes = jnp.where(places < BLK_DEV, places, codes)
        living = places < total
        receivers = jnp.where(living, receivers, 0)
        codes = jnp.where(living, codes, 0)
        return jnp.stack([receivers, codes], axis=-1)
    return jax.vmap(one_group)(subkeys, jnp.arange(SHARDS), counts).astype(jnp.int32)


def with_ends(drawn, rng, smallest, high):
    longest = drawn.shape.index(max(drawn.shape))
    spots = []
    for shift in (0, 1):
        where = [jax.random.randint(jax.random.fold_in(rng, axis), (), 0, length) for axis, length in enumerate(drawn.shape)]
        where[longest] = (where[longest] + shift) % drawn.shape[longest]
        spots.append(tuple(where))
    return drawn.at[spots[0]].set(smallest).at[spots[1]].set(high)


def block_scale(rng, dims, cuts, smallest, largest):
    factor_of, own = 1.0, jax.random.fold_in(rng, 6)
    for dim, blocks in cuts:
        draws = jnp.exp(jax.random.uniform(jax.random.fold_in(own, dim), (blocks,), jnp.float32, smallest / len(cuts), largest / len(cuts)))
        factor_of = factor_of * jnp.repeat(draws, dims[dim] // blocks).reshape([-1 if axis == dim else 1 for axis in range(len(dims))])
    return factor_of


def scatter_about(own_key, extent, spread, bound, shards=(), kind=jnp.bfloat16):
    entries = spread * jax.random.normal(own_key, extent, jnp.float32)
    if shards:
        entries = entries * block_scale(own_key, extent, shards, -0.22, 0.18)
    return jnp.clip(entries, -bound, bound).astype(kind)


def setup_inputs(seed: int = 0) -> dict:
    keys = jax.random.split(jax.random.key(seed), 10)
    return {
        "features": scatter_about(keys[0], (C, ATOMS), 1.0, 6.0, ((0, 8), (1, 64))),
        "positions": draw_positions(jax.random.fold_in(keys[9], 71), 0),
        "block_counts": with_ends(jax.random.randint(keys[2], (BLOCKS,), BLK // 2, BLK + 1), jax.random.fold_in(keys[2], 1), BLK // 2, BLK).astype(jnp.int32),
        "radial_w": scatter_about(keys[3], (NR, 3, C), NR ** -0.5, 2.0, ((2, 8),), jnp.float32),
        "mix_w": scatter_about(keys[4], (4, C, C), (4 * C) ** -0.5, 0.25),
        "read_w": scatter_about(keys[5], (C,), C ** -0.5, 0.5, ((0, 8),), jnp.float32),
        "ghost_lists": draw_ghost_lists(jax.random.fold_in(keys[9], 71), 0),
        "tile_pairs": draw_tile_pairs(jax.random.fold_in(keys[9], 71), 0),
        "tile_count": draw_tile_count(jax.random.fold_in(keys[9], 71), 0),
    }


root_three = 3.0 ** 0.5
root_fifteen = 15.0 ** 0.5
half_root_five = 0.5 * 5.0 ** 0.5
half_root_fifteen = 0.5 * 15.0 ** 0.5
cutoff_square = 9.0
soften = 0.25
center_step = 3.0 / 7.0
radial_sharp = 2.0

def harmonics(unit_x, unit_y, unit_z):
    return jnp.stack([jnp.ones_like(unit_x), root_three * unit_x, root_three * unit_y, root_three * unit_z, root_fifteen * unit_x * unit_y, root_fifteen * unit_y * unit_z, half_root_five * (2.0 * unit_z * unit_z - unit_x * unit_x - unit_y * unit_y), root_fifteen * unit_x * unit_z, half_root_fifteen * (unit_x * unit_x - unit_y * unit_y)])

def tile_kernel(pos_recv, pos_send, self_pair):
    offset = pos_send[:, None, :] - pos_recv[:, :, None]
    dist_sq = lax.optimization_barrier(jnp.sum(offset * offset, axis=0))
    block_width = dist_sq.shape[0]
    diagonal = (lax.broadcasted_iota(jnp.int32, (block_width, block_width), 0) == lax.broadcasted_iota(jnp.int32, (block_width, block_width), 1)).astype(jnp.float32)
    cutoff = jnp.square(jnp.maximum(1.0 - dist_sq / cutoff_square, 0.0)) * (1.0 - self_pair * diagonal)
    distance = jnp.sqrt(dist_sq + soften)
    unit = offset / distance
    angular = harmonics(unit[0], unit[1], unit[2]) * cutoff
    centers = jnp.arange(NR, dtype=jnp.float32) * center_step
    radial = jnp.exp(-radial_sharp * jnp.square(distance[None] - centers[:, None, None]))
    return (radial[:, None] * angular[None]).astype(jnp.bfloat16)

def invariants(density):
    first = density[:, 0]
    return jnp.stack([first, first * first, lax.optimization_barrier(jnp.sum(jnp.square(density[:, 1:4]), axis=1)), lax.optimization_barrier(jnp.sum(jnp.square(density[:, 4:9]), axis=1))])

def reference(features, positions, block_counts, radial_w, mix_w, read_w, ghost_lists, tile_pairs, tile_count):
    present = (jnp.arange(BLK, dtype=jnp.int32)[None, :] < block_counts[:, None]).astype(jnp.float32)
    present_flat = present.reshape(-1)
    senders = (features.astype(jnp.float32) * present_flat[None, :]).astype(jnp.bfloat16)
    send_blocks = senders.reshape(C, BLOCKS, BLK)
    where_blocks = positions.astype(jnp.float32).reshape(3, BLOCKS, BLK)
    degree = jnp.array([0, 1, 1, 1, 2, 2, 2, 2, 2], dtype=jnp.int32)
    table = jnp.take(radial_w, degree, axis=1)
    tile_list = tile_pairs.reshape(SHARDS * TILES_DEV, 2)
    serial = jnp.arange(SHARDS * TILES_DEV, dtype=jnp.int32)
    owners = serial // TILES_DEV
    alive = (serial % TILES_DEV < tile_count[owners]).astype(jnp.float32)
    receivers = (owners * BLK_DEV + tile_list[:, 0]).astype(jnp.int32)
    codes = tile_list[:, 1]
    left_dev = jnp.maximum(owners - 1, 0)
    right_dev = jnp.minimum(owners + 1, SHARDS - 1)
    slot_left = jnp.clip(codes - BLK_DEV, 0, GHOST - 1)
    slot_right = jnp.clip(codes - BLK_DEV - GHOST, 0, GHOST - 1)
    from_left = left_dev * BLK_DEV + ghost_lists[left_dev, 1, slot_left]
    from_right = right_dev * BLK_DEV + ghost_lists[right_dev, 0, slot_right]
    sources = jnp.where(codes < BLK_DEV, owners * BLK_DEV + codes, jnp.where(codes < BLK_DEV + GHOST, from_left, from_right)).astype(jnp.int32)
    self_pairs = ((codes < BLK_DEV) & (codes == tile_list[:, 0])).astype(jnp.float32)

    def update(totals, item):
        receiver, source, self_pair, weight = item
        pos_recv = lax.dynamic_index_in_dim(where_blocks, receiver, 1, keepdims=False)
        pos_send = lax.dynamic_index_in_dim(where_blocks, source, 1, keepdims=False)
        sender_rows = lax.dynamic_index_in_dim(send_blocks, source, 1, keepdims=False)
        kernel = tile_kernel(pos_recv, pos_send, self_pair)
        partial_sums = jnp.einsum('cj,kmij->ckmi', sender_rows.astype(jnp.float32), kernel.astype(jnp.float32))
        term = jnp.einsum('kmc,ckmi->cmi', table, partial_sums, precision=lax.Precision.HIGHEST)
        return (totals.at[receiver].add(term * weight), None)
    start = jnp.zeros((BLOCKS, C, 9, BLK), jnp.float32)
    totals = lax.scan(update, start, (receivers, sources, self_pairs, alive))[0]
    density = totals.transpose(1, 2, 0, 3).reshape(C, 9, ATOMS)
    basis = invariants(density).astype(jnp.bfloat16)
    mixed = jnp.einsum('qco,qca->oa', mix_w.astype(jnp.float32), basis.astype(jnp.float32))
    hidden = features.astype(jnp.float32) + jax.nn.silu(mixed)
    updated = (hidden * present_flat[None, :]).astype(jnp.bfloat16)
    energy = jnp.dot(read_w, hidden, precision=lax.Precision.HIGHEST)
    total_square = jnp.sum(present_flat * energy * energy)
    total_atoms = jnp.sum(present_flat)
    scale = jnp.sqrt(1.0 + total_square / total_atoms)
    return (updated, energy * present_flat / scale, scale)
```

```python
import functools

import jax
import jax.numpy as jnp
from jax import lax
from jax.experimental import pallas as pl
from jax.experimental.pallas import tpu as pltpu
from jax.sharding import PartitionSpec as P

MESH = pl.DeviceIdType.MESH
NR = 8
NM = 9
BLK = 128
OWN = 4
PAIRS = 14

root_three = 3.0**0.5
root_fifteen = 15.0**0.5
half_root_five = 0.5 * 5.0**0.5
half_root_fifteen = 0.5 * 15.0**0.5
cutoff_square = 9.0
soften = 0.25
center_step = 3.0 / 7.0
radial_sharp = 2.0
degree = (0, 1, 1, 1, 2, 2, 2, 2, 2)
order = (0, 2, 1, 3)
place_of = (0, 2, 1, 3)


def kernel(
    na,
    nc,
    feat_hbm,
    pos_hbm,
    counts_hbm,
    radial_hbm,
    mix_hbm,
    read_hbm,
    ghost_hbm,
    pairs_hbm,
    live_hbm,
    upd_out,
    energy_out,
    scale_out,
    feat,
    halo,
    pos,
    mixv,
    mixt,
    rw,
    rd,
    wst,
    wb,
    readcol,
    meta,
    meta_in,
    spos,
    tmat,
    rpos,
    sendt,
    kt,
    run,
    fown,
    ust_send,
    ust,
    est,
    yst,
    xst,
    counts,
    ghost,
    pairs,
    live_count,
    tile_place,
    slot_tile,
    slot_live,
    keep,
    last_slot,
    local_sem,
    feat_send,
    feat_recv,
    w_send,
    w_recv,
    meta_sem,
    halo_send,
    halo_recv,
    u_send,
    u_recv,
    e_send,
    e_recv,
    y_send,
    y_recv,
    x_send,
    x_recv,
):
    cz = feat_hbm.shape[0]
    tiles = pairs.shape[2]
    rows = BLK // nc
    ny = max(1, min(8, na // 2))
    nx = na // (2 * ny)
    nxc = 2 * nx

    g = lax.axis_index("atoms")
    z = lax.axis_index("chan")
    left, right = lax.rem(g + na - 1, na), lax.rem(g + 1, na)
    xi = g // (2 * ny)
    yi = lax.rem(g // 2, ny)
    ci = lax.rem(g, 2)
    xc = xi * 2 + ci

    def chan_peer(d):
        return (g, lax.rem(z + d, nc))

    def y_peer(d):
        return (xi * (2 * ny) + lax.rem(yi + d, ny) * 2 + ci, z)

    def x_peer(d):
        other = lax.rem(xc + d, nxc)
        return ((other // 2) * (2 * ny) + yi * 2 + lax.rem(other, 2), z)

    own_rows = pl.ds(pl.multiple_of(z * cz, cz), cz)

    local = [
        pltpu.make_async_copy(
            feat_hbm.at[:, pl.ds(BLK * b, BLK)],
            feat.at[own_rows, pl.ds(BLK * n, BLK)],
            local_sem.at[n],
        )
        for n, b in enumerate(order)
    ]
    pos_copy = pltpu.make_async_copy(pos_hbm, pos, local_sem.at[4])
    rw_copy = pltpu.make_async_copy(radial_hbm, rw, local_sem.at[5])
    rd_copy = pltpu.make_async_copy(read_hbm, rd, local_sem.at[6])
    mix_copy = pltpu.make_async_copy(mix_hbm, mixv, local_sem.at[7])
    ints = [
        pltpu.make_async_copy(src, dst, local_sem.at[8 + n])
        for n, (src, dst) in enumerate(
            ((counts_hbm, counts), (ghost_hbm, ghost), (pairs_hbm, pairs), (live_hbm, live_count))
        )
    ]
    pos_copy.start()
    for c in ints:
        c.start()
    for c in local:
        c.start()
    rw_copy.start()
    rd_copy.start()
    mix_copy.start()

    barrier = pltpu.get_barrier_semaphore()
    greeted = 0
    for d in range(1, nc):
        pl.semaphore_signal(barrier, inc=1, device_id=chan_peer(d), device_id_type=MESH)
        greeted += 1
    for other in (left, right):
        pl.semaphore_signal(barrier, inc=1, device_id=(other, z), device_id_type=MESH)
        greeted += 1
    for d in range(1, ny):
        pl.semaphore_signal(barrier, inc=1, device_id=y_peer(d), device_id_type=MESH)
        greeted += 1
    for d in range(1, nxc):
        pl.semaphore_signal(barrier, inc=1, device_id=x_peer(d), device_id_type=MESH)
        greeted += 1

    lane = lax.broadcasted_iota(jnp.int32, (1, BLK), 1)
    for c in ints:
        c.wait()
    pos_copy.wait()
    zero_row = jnp.zeros((1, BLK), jnp.float32)
    boxes = []
    for b in range(OWN):
        where = pos[:, pl.ds(BLK * b, BLK)]
        present = (lane < counts[b]).astype(jnp.float32)
        low = (ghost[0, 0, 0] >> 1).astype(jnp.float32)
        high = (ghost[0, 1, 0] >> 1).astype(jnp.float32)
        rows8 = jnp.concatenate(
            [where, present, zero_row + low, zero_row + high, zero_row, zero_row], axis=0
        )
        boxes.append(rows8)
        spos[b] = rows8
    swap_low = ghost[0, 0, 0] != 0
    swap_high = ghost[0, 1, 0] != 1
    meta[0, 0] = jnp.where(swap_low, boxes[2], boxes[0])
    meta[0, 1] = jnp.where(swap_low, boxes[0], boxes[2])
    meta[1, 0] = jnp.where(swap_high, boxes[3], boxes[1])
    meta[1, 1] = jnp.where(swap_high, boxes[1], boxes[3])

    rw_copy.wait()
    rd_copy.wait()
    folded = jnp.concatenate([rw[:, k, :] for k in range(NR)], axis=1)
    read_row = jnp.concatenate(
        [rd[...].reshape(1, cz), jnp.zeros((1, BLK - cz), jnp.float32)], axis=1
    )
    wst[z] = jnp.concatenate([folded, read_row, jnp.zeros((4, BLK), jnp.float32)], axis=0)

    total = live_count[0]

    def count(t, acc):
        r = pairs[0, 0, t]
        alive = t < total
        rank = jnp.int32(0)
        out = []
        for b in range(OWN):
            hit = jnp.logical_and(alive, r == b)
            rank = jnp.where(hit, acc[b], rank)
            out.append(acc[b] + hit.astype(jnp.int32))
        tile_place[t] = rank
        return tuple(out)

    sizes = lax.fori_loop(0, tiles, count, (jnp.int32(0),) * OWN)
    starts = [jnp.int32(0)]
    for b in range(OWN):
        used = (sizes[b] + 1) >> 1
        last_slot[b] = jnp.maximum(starts[b] + used - 1, 0)
        starts.append(starts[b] + used)

    def settle(t, _):
        r = pairs[0, 0, t]
        first = jnp.int32(0)
        for b in range(OWN):
            first = jnp.where(r == b, starts[b], first)
        spot = 2 * first + tile_place[t]
        tile_place[t] = jnp.where(t < total, spot, -1)
        return 0

    lax.fori_loop(0, tiles, settle, 0)

    def fill(s, _):
        which, alive = jnp.int32(0), jnp.int32(0)
        for t in range(tiles):
            hit = (tile_place[t] == s).astype(jnp.int32)
            which = which + hit * t
            alive = alive + hit
        slot_tile[s] = which
        slot_live[s] = alive
        return 0

    lax.fori_loop(0, 2 * PAIRS, fill, 0)

    def mark(p, _):
        same = jnp.int32(1)
        for b in range(OWN):
            same = jnp.where(starts[b] == p, 0, same)
        keep[p] = same
        return 0

    lax.fori_loop(0, PAIRS, mark, 0)

    tmat[...] = jnp.zeros((BLK, BLK), jnp.float32)
    for b in range(OWN):
        tmat[pl.ds(8 * b, 8), :] = boxes[b]
    tmat[...] = tmat[...].T
    mine = tmat[pl.ds(pl.multiple_of(z * rows, rows), rows), :]
    for b in range(OWN):
        for d in range(3):
            rpos[b, d] = jnp.broadcast_to(mine[:, 8 * b + d : 8 * b + d + 1], (rows, BLK))

    for c in local:
        c.wait()
    pl.semaphore_wait(barrier, greeted)

    def feat_copy(d):
        return pltpu.make_async_remote_copy(
            src_ref=feat.at[own_rows],
            dst_ref=feat.at[own_rows],
            send_sem=feat_send.at[d],
            recv_sem=feat_recv.at[d],
            device_id=chan_peer(d),
            device_id_type=MESH,
        )

    def w_copy(d):
        return pltpu.make_async_remote_copy(
            src_ref=wst.at[z],
            dst_ref=wst.at[z],
            send_sem=w_send.at[d],
            recv_sem=w_recv.at[d],
            device_id=chan_peer(d),
            device_id_type=MESH,
        )

    def meta_copy(side):
        return pltpu.make_async_remote_copy(
            src_ref=meta.at[side],
            dst_ref=meta_in.at[1 - side],
            send_sem=meta_sem.at[side],
            recv_sem=meta_sem.at[3 - side],
            device_id=(left if side == 0 else right, z),
            device_id_type=MESH,
        )

    def halo_copy(side, d):
        part = pl.ds(pl.multiple_of(lax.rem(z + nc - d, nc) * cz, cz), cz)
        return pltpu.make_async_remote_copy(
            src_ref=feat.at[part, pl.ds(2 * BLK * side, 2 * BLK)],
            dst_ref=halo.at[1 - side, part],
            send_sem=halo_send.at[side, d],
            recv_sem=halo_recv.at[1 - side, d],
            device_id=(left if side == 0 else right, z),
            device_id_type=MESH,
        )

    far_first = sorted(range(1, nc), key=lambda d: -min(d, nc - d))
    near_first = far_first[::-1]
    for side in range(2):
        meta_copy(side).start()
    for d in far_first:
        feat_copy(d).start()
    for side in range(2):
        halo_copy(side, 0).start()
    for d in far_first:
        w_copy(d).start()

    for side in range(2):
        meta_copy(side).wait_recv()
    for side in range(2):
        for n in range(2):
            spos[OWN + 2 * side + n] = meta_in[side, n]

    shape = (rows, BLK)
    own_index = lax.broadcasted_iota(jnp.int32, shape, 0) + z * rows
    off_diagonal = (own_index != lax.broadcasted_iota(jnp.int32, shape, 1)).astype(jnp.float32)

    def geometry(p, half):
        s = 2 * p + half
        t = slot_tile[s]
        r = pairs[0, 0, t]
        q = pairs[0, 1, t]
        there = spos[q]
        weight = slot_live[s].astype(jnp.float32)
        own = (q == r).astype(jnp.float32)
        off = [there[d : d + 1, :] - rpos[r, d] for d in range(3)]
        dist_sq = off[0] * off[0] + off[1] * off[1] + off[2] * off[2]
        shut = jnp.square(jnp.maximum(1.0 - dist_sq / cutoff_square, 0.0))
        shut = shut * (1.0 - own * (1.0 - off_diagonal))
        shut = shut * (there[3:4, :] * weight)
        distance = jnp.sqrt(dist_sq + soften)
        inverse = 1.0 / distance
        ux, uy, uz = (o * inverse for o in off)
        angular = (
            None,
            root_three * ux,
            root_three * uy,
            root_three * uz,
            root_fifteen * ux * uy,
            root_fifteen * uy * uz,
            half_root_five * (2.0 * uz * uz - ux * ux - uy * uy),
            root_fifteen * ux * uz,
            half_root_fifteen * (ux * ux - uy * uy),
        )
        angular = [shut if y is None else y * shut for y in angular]
        for k in range(NR):
            radial = jnp.exp(-radial_sharp * jnp.square(distance - k * center_step))
            for m in range(NM):
                kt[p, pl.ds((m * NR + k) * rows, rows), pl.ds(BLK * half, BLK)] = (
                    radial * angular[m]
                ).astype(jnp.bfloat16)

    def two_pairs(step):
        def one(p, _):
            for half in range(2):
                geometry(p, half)
            return 0

        lax.fori_loop(2 * step, 2 * step + 2, one, 0)

    for step, d in enumerate(near_first):
        two_pairs(step)
        feat_copy(d).wait_recv()
        for side in range(2):
            halo_copy(side, d).start()

    for b in range(OWN):
        sendt[b] = feat[:, pl.ds(BLK * place_of[b], BLK)].T
    shift = lax.rem(BLK - z * rows, BLK)
    fown[...] = jnp.concatenate(
        [
            pltpu.roll(feat[:, pl.ds(BLK * place_of[b], BLK)].astype(jnp.float32), shift, 1)[:, :rows]
            for b in range(OWN)
        ]
        + [jnp.zeros((BLK, BLK - OWN * rows), jnp.float32)],
        axis=1,
    )
    own_present = jnp.concatenate(
        [pltpu.roll(boxes[b], shift, 1)[3:4, :rows] for b in range(OWN)]
        + [jnp.zeros((1, BLK - OWN * rows), jnp.float32)],
        axis=1,
    )
    mix_copy.wait()
    for n in range(4):
        mixt[:, pl.ds(BLK * n, BLK)] = mixv[n].T
    for d in range(1, nc):
        w_copy(d).wait_recv()
    for k in range(NR):
        whole = jnp.concatenate([wst[s, :, cz * k : cz * (k + 1)] for s in range(nc)], axis=1)
        for l in range(3):
            wb[l, k] = jnp.broadcast_to(whole[l : l + 1, :], (8, BLK))
        if k == 0:
            readcol[...] = jnp.broadcast_to(whole[3:4, :], (BLK, BLK)).T
    for d in range(nc):
        for side in range(2):
            halo_copy(side, d).wait_recv()
    for side in range(2):
        bit = meta_in[side, 0][5 - side : 6 - side, :] > 0.5
        early = halo[side, :, 0:BLK].astype(jnp.float32)
        late = halo[side, :, BLK : 2 * BLK].astype(jnp.float32)
        sendt[OWN + 2 * side] = jnp.where(bit, late, early).astype(jnp.bfloat16).T
        sendt[OWN + 2 * side + 1] = jnp.where(bit, early, late).astype(jnp.bfloat16).T

    run[PAIRS] = jnp.zeros((NM * rows, BLK), jnp.float32)

    def message(p, _):
        q0 = pairs[0, 1, slot_tile[2 * p]]
        q1 = pairs[0, 1, slot_tile[2 * p + 1]]
        both = jnp.concatenate([sendt[q0], sendt[q1]], axis=0)
        before = lax.rem(p + PAIRS, PAIRS + 1)
        kept = keep[p].astype(jnp.float32)
        part = jnp.dot(kt[p], both, preferred_element_type=jnp.float32)
        for m in range(NM):
            acc = run[before, pl.ds(m * rows, rows), :] * kept
            for k in range(NR):
                w = wb[degree[m], k]
                at = (m * NR + k) * rows
                acc = acc + jnp.concatenate([w] * (rows // 8), axis=0) * part[at : at + rows, :]
            run[p, pl.ds(m * rows, rows), :] = acc
        return 0

    lax.fori_loop(0, PAIRS, message, 0)

    basis = []
    for b in range(OWN):
        slot = last_slot[b]
        den = [run[slot, pl.ds(m * rows, rows), :] for m in range(NM)]
        vec = den[1] * den[1] + den[2] * den[2] + den[3] * den[3]
        ten = sum(den[m] * den[m] for m in range(5, NM)) + den[4] * den[4]
        basis.append(jnp.concatenate([den[0], den[0] * den[0], vec, ten], axis=1))
    basis = jnp.concatenate(
        basis + [jnp.zeros((BLK - OWN * rows, 4 * BLK), jnp.float32)], axis=0
    ).astype(jnp.bfloat16)
    mixed = lax.dot_general(
        mixt[...], basis, (((1,), (1,)), ((), ())), preferred_element_type=jnp.float32
    )
    hidden = fown[...] + mixed / (1.0 + jnp.exp(-mixed))
    energy = jnp.sum(readcol[...] * hidden, axis=0, keepdims=True)
    square = jnp.sum(energy * energy * own_present, axis=1, keepdims=True)
    est[z] = jnp.concatenate(
        [energy, jnp.broadcast_to(square, (1, BLK)), jnp.zeros((6, BLK), jnp.float32)], axis=0
    )

    def e_copy(d):
        return pltpu.make_async_remote_copy(
            src_ref=est.at[z],
            dst_ref=est.at[z],
            send_sem=e_send.at[d],
            recv_sem=e_recv.at[d],
            device_id=chan_peer(d),
            device_id_type=MESH,
        )

    def u_copy(d):
        part = pl.ds(pl.multiple_of(lax.rem(z + d, nc) * cz, cz), cz)
        return pltpu.make_async_remote_copy(
            src_ref=ust_send.at[part],
            dst_ref=ust.at[z],
            send_sem=u_send.at[d],
            recv_sem=u_recv.at[d],
            device_id=chan_peer(d),
            device_id_type=MESH,
        )

    for d in far_first:
        e_copy(d).start()
    ust_send[...] = (hidden * own_present).astype(jnp.bfloat16)
    ust[z] = ust_send[own_rows, :]
    for d in range(1, nc):
        e_copy(d).wait_recv()
    group = est[0, 1:2, :]
    for s in range(1, nc):
        group = group + est[s, 1:2, :]
    atoms = zero_row
    for b in range(OWN):
        atoms = atoms + counts[b].astype(jnp.float32)
    fill6 = jnp.zeros((6, BLK), jnp.float32)
    yst[yi] = jnp.concatenate([group, atoms, fill6], axis=0)

    def y_copy(d):
        return pltpu.make_async_remote_copy(
            src_ref=yst.at[yi],
            dst_ref=yst.at[yi],
            send_sem=y_send.at[d],
            recv_sem=y_recv.at[d],
            device_id=y_peer(d),
            device_id_type=MESH,
        )

    def x_copy(d):
        return pltpu.make_async_remote_copy(
            src_ref=xst.at[xc],
            dst_ref=xst.at[xc],
            send_sem=x_send.at[d],
            recv_sem=x_recv.at[d],
            device_id=x_peer(d),
            device_id_type=MESH,
        )

    for d in range(1, ny):
        y_copy(d).start()
    for d in far_first:
        u_copy(d).start()
    energies = []
    for b in range(OWN):
        line = jnp.concatenate(
            [est[s, 0:1, rows * b : rows * (b + 1)] for s in range(nc)], axis=1
        )
        energies.append(line * boxes[b][3:4, :])
    energies = jnp.concatenate(energies, axis=0)
    for d in range(1, ny):
        y_copy(d).wait_recv()
    plane = yst[0]
    for s in range(1, ny):
        plane = plane + yst[s]
    xst[xc] = plane
    for d in range(1, nxc):
        x_copy(d).start()
    for d in range(1, nc):
        u_copy(d).wait_recv()
    for b in range(OWN):
        upd_out[:, pl.ds(BLK * b, BLK)] = jnp.concatenate(
            [ust[s].astype(jnp.float32)[:, rows * b : rows * (b + 1)] for s in range(nc)], axis=1
        ).astype(jnp.bfloat16)
    for d in range(1, nxc):
        x_copy(d).wait_recv()
    whole = xst[0]
    for s in range(1, nxc):
        whole = whole + xst[s]
    scale = jnp.sqrt(1.0 + whole[0:1, :] / whole[1:2, :])
    energy_out[...] = energies / scale
    scale_out[...] = scale

    for side in range(2):
        meta_copy(side).wait_send()
        for d in range(nc):
            halo_copy(side, d).wait_send()
    for d in range(1, nc):
        feat_copy(d).wait_send()
        w_copy(d).wait_send()
        e_copy(d).wait_send()
        u_copy(d).wait_send()
    for d in range(1, ny):
        y_copy(d).wait_send()
    for d in range(1, nxc):
        x_copy(d).wait_send()


def per_device(
    na, nc, features, positions, block_counts, radial_w, mix_w, read_w, ghost_lists, tile_pairs, tile_count
):
    cz, width = features.shape
    rows = BLK // nc
    ny = max(1, min(8, na // 2))
    nxc = na // ny
    tiles = tile_pairs.shape[1]
    radial_w = radial_w.transpose(1, 0, 2)
    tile_pairs = tile_pairs.transpose(0, 2, 1)
    f32, bf16, i32 = jnp.float32, jnp.bfloat16, jnp.int32
    vm, sm, dma = pltpu.VMEM, pltpu.SMEM, pltpu.SemaphoreType.DMA
    hbm = pl.BlockSpec(memory_space=pltpu.HBM)
    vmem = pl.BlockSpec(memory_space=pltpu.VMEM)
    updated, energies, scale = pl.pallas_call(
        functools.partial(kernel, na, nc),
        out_shape=(
            jax.ShapeDtypeStruct((cz, width), bf16),
            jax.ShapeDtypeStruct((OWN, BLK), f32),
            jax.ShapeDtypeStruct((1, BLK), f32),
        ),
        in_specs=[hbm] * 9,
        out_specs=(vmem, vmem, vmem),
        scratch_shapes=[
            vm((BLK, width), bf16),
            vm((2, BLK, 2 * BLK), bf16),
            vm((3, width), f32),
            vm((4, BLK, BLK), bf16),
            vm((BLK, 4 * BLK), bf16),
            vm((3, NR, cz), f32),
            vm((cz,), f32),
            vm((nc, 8, BLK), f32),
            vm((3, NR, 8, BLK), f32),
            vm((BLK, BLK), f32),
            vm((2, 2, 8, BLK), f32),
            vm((2, 2, 8, BLK), f32),
            vm((2 * OWN, 8, BLK), f32),
            vm((BLK, BLK), f32),
            vm((OWN, 3, rows, BLK), f32),
            vm((2 * OWN, BLK, BLK), bf16),
            vm((PAIRS, NM * NR * rows, 2 * BLK), bf16),
            vm((PAIRS + 1, NM * rows, BLK), f32),
            vm((BLK, BLK), f32),
            vm((BLK, BLK), bf16),
            vm((nc, cz, BLK), bf16),
            vm((nc, 8, BLK), f32),
            vm((ny, 8, BLK), f32),
            vm((nxc, 8, BLK), f32),
            sm((OWN,), i32),
            sm((1, 2, 2), i32),
            sm((1, 2, tiles), i32),
            sm((1,), i32),
            sm((tiles,), i32),
            sm((2 * PAIRS,), i32),
            sm((2 * PAIRS,), i32),
            sm((PAIRS,), i32),
            sm((OWN,), i32),
            dma((12,)),
            dma((nc,)),
            dma((nc,)),
            dma((nc,)),
            dma((nc,)),
            dma((4,)),
            dma((2, nc)),
            dma((2, nc)),
            dma((nc,)),
            dma((nc,)),
            dma((nc,)),
            dma((nc,)),
            dma((max(ny, 2),)),
            dma((max(ny, 2),)),
            dma((max(nxc, 2),)),
            dma((max(nxc, 2),)),
        ],
        compiler_params=pltpu.CompilerParams(
            collective_id=0, has_side_effects=True, vmem_limit_bytes=67043328
        ),
        name="message_layer",
    )(features, positions, block_counts, radial_w, mix_w, read_w, ghost_lists, tile_pairs, tile_count)
    return updated, energies.reshape(width), scale[0, 0]


def solution(mesh):
    in_specs = (
        P("chan", "atoms"),
        P(None, "atoms"),
        P("atoms"),
        P(None, None, "chan"),
        P(),
        P("chan"),
        P("atoms", None, None),
        P("atoms", None, None),
        P("atoms"),
    )
    out_specs = (P("chan", "atoms"), P("atoms"), P())
    step = functools.partial(per_device, mesh.shape["atoms"], mesh.shape["chan"])
    return jax.shard_map(step, mesh=mesh, in_specs=in_specs, out_specs=out_specs, check_vma=False)
```

```python
import functools

import jax
import jax.numpy as jnp
from jax import lax
from jax.experimental import pallas as pl
from jax.experimental.pallas import tpu as pltpu
from jax.sharding import PartitionSpec as P

MESH = pl.DeviceIdType.MESH
NR = 8
NM = 9
BLK = 128
OWN = 4
PAIRS = 14

root_three = 3.0**0.5
root_fifteen = 15.0**0.5
half_root_five = 0.5 * 5.0**0.5
half_root_fifteen = 0.5 * 15.0**0.5
cutoff_square = 9.0
soften = 0.25
center_step = 3.0 / 7.0
radial_sharp = 2.0
degree = (0, 1, 1, 1, 2, 2, 2, 2, 2)
order = (0, 2, 1, 3)
place_of = (0, 2, 1, 3)


def kernel(
    na,
    nc,
    feat_hbm,
    pos_hbm,
    counts_hbm,
    radial_hbm,
    mix_hbm,
    read_hbm,
    ghost_hbm,
    pairs_hbm,
    live_hbm,
    upd_out,
    energy_out,
    scale_out,
    feat,
    halo,
    pos,
    mixv,
    mixt,
    rw,
    rd,
    wst,
    wb,
    readcol,
    meta,
    meta_in,
    spos,
    tmat,
    rpos,
    sendt,
    kt,
    run,
    fown,
    ust_send,
    ust,
    est,
    plane,
    counts,
    ghost,
    pairs,
    live_count,
    tile_place,
    slot_tile,
    slot_live,
    keep,
    last_slot,
    local_sem,
    feat_send,
    feat_recv,
    w_send,
    w_recv,
    meta_sem,
    halo_send,
    halo_recv,
    u_send,
    u_recv,
    e_send,
    e_recv,
    plane_sem,
    ready,
):
    cz = feat_hbm.shape[0]
    tiles = pairs.shape[2]
    rows = BLK // nc
    ny = max(1, min(8, na // 2))
    nx = na // (2 * ny)
    nxc = 2 * nx

    g = lax.axis_index("atoms")
    z = lax.axis_index("chan")
    left, right = lax.rem(g + na - 1, na), lax.rem(g + 1, na)
    xi = g // (2 * ny)
    yi = lax.rem(g // 2, ny)
    ci = lax.rem(g, 2)
    xc = xi * 2 + ci

    def chan_peer(d):
        return (g, lax.rem(z + d, nc))

    def y_peer(d):
        return (xi * (2 * ny) + lax.rem(yi + d, ny) * 2 + ci, z)

    def x_peer(d):
        other = lax.rem(xc + d, nxc)
        return ((other // 2) * (2 * ny) + yi * 2 + lax.rem(other, 2), z)

    own_rows = pl.ds(pl.multiple_of(z * cz, cz), cz)

    barrier = pltpu.get_barrier_semaphore()
    greeted = 0
    for d in range(1, nc):
        pl.semaphore_signal(barrier, inc=1, device_id=chan_peer(d), device_id_type=MESH)
        greeted += 1
    for other in (left, right):
        pl.semaphore_signal(barrier, inc=1, device_id=(other, z), device_id_type=MESH)
        greeted += 1
    for d in range(1, ny):
        pl.semaphore_signal(barrier, inc=1, device_id=y_peer(d), device_id_type=MESH)
        greeted += 1
    for d in range(1, nxc):
        pl.semaphore_signal(barrier, inc=1, device_id=x_peer(d), device_id_type=MESH)
        greeted += 1

    local = [
        pltpu.make_async_copy(
            feat_hbm.at[:, pl.ds(BLK * b, BLK)],
            feat.at[own_rows, pl.ds(BLK * n, BLK)],
            local_sem.at[n],
        )
        for n, b in enumerate(order)
    ]
    pos_copy = pltpu.make_async_copy(pos_hbm, pos, local_sem.at[4])
    rw_copy = pltpu.make_async_copy(radial_hbm, rw, local_sem.at[5])
    rd_copy = pltpu.make_async_copy(read_hbm, rd, local_sem.at[6])
    mix_copy = pltpu.make_async_copy(mix_hbm, mixv, local_sem.at[7])
    ints = [
        pltpu.make_async_copy(src, dst, local_sem.at[8 + n])
        for n, (src, dst) in enumerate(
            ((counts_hbm, counts), (ghost_hbm, ghost), (pairs_hbm, pairs), (live_hbm, live_count))
        )
    ]
    for c in local:
        c.start()
    pos_copy.start()
    for c in ints:
        c.start()
    rw_copy.start()
    rd_copy.start()
    mix_copy.start()

    lane = lax.broadcasted_iota(jnp.int32, (1, BLK), 1)
    for c in ints:
        c.wait()
    pos_copy.wait()
    zero_row = jnp.zeros((1, BLK), jnp.float32)
    boxes = []
    for b in range(OWN):
        where = pos[:, pl.ds(BLK * b, BLK)]
        present = (lane < counts[b]).astype(jnp.float32)
        low = (ghost[0, 0, 0] >> 1).astype(jnp.float32)
        high = (ghost[0, 1, 0] >> 1).astype(jnp.float32)
        rows8 = jnp.concatenate(
            [where, present, zero_row + low, zero_row + high, zero_row, zero_row], axis=0
        )
        boxes.append(rows8)
        spos[b] = rows8
    swap_low = ghost[0, 0, 0] != 0
    swap_high = ghost[0, 1, 0] != 1
    meta[0, 0] = jnp.where(swap_low, boxes[2], boxes[0])
    meta[0, 1] = jnp.where(swap_low, boxes[0], boxes[2])
    meta[1, 0] = jnp.where(swap_high, boxes[3], boxes[1])
    meta[1, 1] = jnp.where(swap_high, boxes[1], boxes[3])

    rw_copy.wait()
    rd_copy.wait()
    folded = jnp.concatenate([rw[:, k, :] for k in range(NR)], axis=1)
    read_row = jnp.concatenate(
        [rd[...].reshape(1, cz), jnp.zeros((1, BLK - cz), jnp.float32)], axis=1
    )
    wst[z] = jnp.concatenate([folded, read_row, jnp.zeros((4, BLK), jnp.float32)], axis=0)

    total = live_count[0]

    sizes = [jnp.int32(0)] * OWN
    ranks = []
    for t in range(tiles):
        r = pairs[0, 0, t]
        alive = (t < total).astype(jnp.int32)
        rank = sizes[0]
        for b in range(1, OWN):
            rank = jnp.where(r == b, sizes[b], rank)
        ranks.append(rank)
        sizes = [n + jnp.where(r == b, alive, 0) for b, n in enumerate(sizes)]
    starts = [jnp.int32(0)]
    for b in range(OWN):
        used = (sizes[b] + 1) >> 1
        last_slot[b] = jnp.maximum(starts[b] + used - 1, 0)
        starts.append(starts[b] + used)
    for t in range(tiles):
        r = pairs[0, 0, t]
        first = starts[0]
        for b in range(1, OWN):
            first = jnp.where(r == b, starts[b], first)
        tile_place[t] = jnp.where(t < total, 2 * first + ranks[t], -1)

    for p in range(PAIRS):
        same = jnp.int32(1)
        for b in range(OWN):
            same = jnp.where(starts[b] == p, 0, same)
        keep[p] = same

    def fill(n, _):
        found = [jnp.int32(0)] * 4
        for t in range(tiles):
            place = tile_place[t]
            found = [jnp.where(place == 4 * n + u, t + 32, f) for u, f in enumerate(found)]
        for u, f in enumerate(found):
            slot_tile[4 * n + u] = f & 31
            slot_live[4 * n + u] = f >> 5
        return 0

    lax.fori_loop(0, PAIRS // 2, fill, 0)

    for c in local:
        c.wait()
    pl.semaphore_wait(barrier, greeted)

    def feat_copy(d):
        return pltpu.make_async_remote_copy(
            src_ref=feat.at[own_rows],
            dst_ref=feat.at[own_rows],
            send_sem=feat_send.at[d],
            recv_sem=feat_recv.at[d],
            device_id=chan_peer(d),
            device_id_type=MESH,
        )

    def w_copy(d):
        return pltpu.make_async_remote_copy(
            src_ref=wst.at[z],
            dst_ref=wst.at[z],
            send_sem=w_send.at[d],
            recv_sem=w_recv.at[d],
            device_id=chan_peer(d),
            device_id_type=MESH,
        )

    def meta_copy(side):
        return pltpu.make_async_remote_copy(
            src_ref=meta.at[side],
            dst_ref=meta_in.at[1 - side],
            send_sem=meta_sem.at[side],
            recv_sem=meta_sem.at[3 - side],
            device_id=(left if side == 0 else right, z),
            device_id_type=MESH,
        )

    def halo_copy(side, d):
        part = pl.ds(pl.multiple_of(lax.rem(z + nc - d, nc) * cz, cz), cz)
        return pltpu.make_async_remote_copy(
            src_ref=feat.at[part, pl.ds(2 * BLK * side, 2 * BLK)],
            dst_ref=halo.at[1 - side, part],
            send_sem=halo_send.at[side, d],
            recv_sem=halo_recv.at[1 - side, d],
            device_id=(left if side == 0 else right, z),
            device_id_type=MESH,
        )

    far_first = sorted(range(1, nc), key=lambda d: -min(d, nc - d))
    near_first = far_first[::-1]
    for d in far_first:
        feat_copy(d).start()
    for side in range(2):
        halo_copy(side, 0).start()
    for side in range(2):
        meta_copy(side).start()
    for d in far_first:
        w_copy(d).start()
    for d in range(1, ny):
        pl.semaphore_signal(ready, inc=1, device_id=y_peer(d), device_id_type=MESH)

    tmat[...] = jnp.zeros((BLK, BLK), jnp.float32)
    for b in range(OWN):
        tmat[pl.ds(8 * b, 8), :] = boxes[b]
    tmat[...] = tmat[...].T
    mine = tmat[pl.ds(pl.multiple_of(z * rows, rows), rows), :]
    for b in range(OWN):
        for d in range(3):
            rpos[b, d] = jnp.broadcast_to(mine[:, 8 * b + d : 8 * b + d + 1], (rows, BLK))

    for side in range(2):
        meta_copy(side).wait_recv()
    for side in range(2):
        for n in range(2):
            spos[OWN + 2 * side + n] = meta_in[side, n]

    shape = (rows, BLK)
    own_index = lax.broadcasted_iota(jnp.int32, shape, 0) + z * rows
    off_diagonal = (own_index != lax.broadcasted_iota(jnp.int32, shape, 1)).astype(jnp.float32)

    def geometry(p, half):
        s = 2 * p + half
        t = slot_tile[s]
        r = pairs[0, 0, t]
        q = pairs[0, 1, t]
        there = spos[q]
        weight = slot_live[s].astype(jnp.float32)
        own = (q == r).astype(jnp.float32)
        off = [there[d : d + 1, :] - rpos[r, d] for d in range(3)]
        dist_sq = off[0] * off[0] + off[1] * off[1] + off[2] * off[2]
        shut = jnp.square(jnp.maximum(1.0 - dist_sq / cutoff_square, 0.0))
        shut = shut * (1.0 - own * (1.0 - off_diagonal))
        shut = shut * (there[3:4, :] * weight)
        distance = jnp.sqrt(dist_sq + soften)
        inverse = 1.0 / distance
        ux, uy, uz = (o * inverse for o in off)
        angular = (
            None,
            root_three * ux,
            root_three * uy,
            root_three * uz,
            root_fifteen * ux * uy,
            root_fifteen * uy * uz,
            half_root_five * (2.0 * uz * uz - ux * ux - uy * uy),
            root_fifteen * ux * uz,
            half_root_fifteen * (ux * ux - uy * uy),
        )
        angular = [shut if y is None else y * shut for y in angular]
        for k in range(NR):
            radial = jnp.exp(-radial_sharp * jnp.square(distance - k * center_step))
            for m in range(NM):
                kt[p, pl.ds((m * NR + k) * rows, rows), pl.ds(BLK * half, BLK)] = (
                    radial * angular[m]
                ).astype(jnp.bfloat16)

    def two_pairs(step):
        def one(p, _):
            for half in range(2):
                geometry(p, half)
            return 0

        lax.fori_loop(2 * step, 2 * step + 2, one, 0)

    for step, d in enumerate(near_first):
        two_pairs(step)
        feat_copy(d).wait_recv()
        for side in range(2):
            halo_copy(side, d).start()

    for b in range(OWN):
        sendt[b] = feat[:, pl.ds(BLK * place_of[b], BLK)].T
    shift = lax.rem(BLK - z * rows, BLK)
    fown[...] = jnp.concatenate(
        [
            pltpu.roll(feat[:, pl.ds(BLK * place_of[b], BLK)].astype(jnp.float32), shift, 1)[:, :rows]
            for b in range(OWN)
        ]
        + [jnp.zeros((BLK, BLK - OWN * rows), jnp.float32)],
        axis=1,
    )
    own_present = jnp.concatenate(
        [pltpu.roll(boxes[b], shift, 1)[3:4, :rows] for b in range(OWN)]
        + [jnp.zeros((1, BLK - OWN * rows), jnp.float32)],
        axis=1,
    )
    mix_copy.wait()
    for n in range(4):
        mixt[:, pl.ds(BLK * n, BLK)] = mixv[n].T
    for d in range(1, nc):
        w_copy(d).wait_recv()
    for k in range(NR):
        whole = jnp.concatenate([wst[s, :, cz * k : cz * (k + 1)] for s in range(nc)], axis=1)
        for l in range(3):
            wb[l, k] = jnp.broadcast_to(whole[l : l + 1, :], (8, BLK))
        if k == 0:
            readcol[...] = jnp.broadcast_to(whole[3:4, :], (BLK, BLK)).T
    for d in range(nc):
        for side in range(2):
            halo_copy(side, d).wait_recv()
    for side in range(2):
        bit = meta_in[side, 0][5 - side : 6 - side, :] > 0.5
        early = halo[side, :, 0:BLK].astype(jnp.float32)
        late = halo[side, :, BLK : 2 * BLK].astype(jnp.float32)
        sendt[OWN + 2 * side] = jnp.where(bit, late, early).astype(jnp.bfloat16).T
        sendt[OWN + 2 * side + 1] = jnp.where(bit, early, late).astype(jnp.bfloat16).T

    def message(p):
        q0 = pairs[0, 1, slot_tile[2 * p]]
        q1 = pairs[0, 1, slot_tile[2 * p + 1]]
        both = jnp.concatenate([sendt[q0], sendt[q1]], axis=0)
        kept = keep[p].astype(jnp.float32)
        part = jnp.dot(kt[p], both, preferred_element_type=jnp.float32)
        for m in range(NM):
            acc = 0.0 if p == 0 else run[p - 1, pl.ds(m * rows, rows), :] * kept
            for k in range(NR):
                w = wb[degree[m], k]
                at = (m * NR + k) * rows
                acc = acc + jnp.concatenate([w] * (rows // 8), axis=0) * part[at : at + rows, :]
            run[p, pl.ds(m * rows, rows), :] = acc

    for p in range(PAIRS):
        message(p)

    basis = []
    for b in range(OWN):
        slot = last_slot[b]
        den = [run[slot, pl.ds(m * rows, rows), :] for m in range(NM)]
        vec = den[1] * den[1] + den[2] * den[2] + den[3] * den[3]
        ten = sum(den[m] * den[m] for m in range(5, NM)) + den[4] * den[4]
        basis.append(jnp.concatenate([den[0], den[0] * den[0], vec, ten], axis=1))
    basis = jnp.concatenate(
        basis + [jnp.zeros((BLK - OWN * rows, 4 * BLK), jnp.float32)], axis=0
    ).astype(jnp.bfloat16)
    mixed = lax.dot_general(
        mixt[...], basis, (((1,), (1,)), ((), ())), preferred_element_type=jnp.float32
    )
    hidden = fown[...] + mixed / (1.0 + jnp.exp(-mixed))
    energy = jnp.sum(readcol[...] * hidden, axis=0, keepdims=True)
    square = jnp.sum(energy * energy * own_present, axis=1, keepdims=True)
    est[z] = jnp.where(lane < OWN * rows, energy, jnp.broadcast_to(square, (1, BLK)))

    def e_copy(d):
        return pltpu.make_async_remote_copy(
            src_ref=est.at[z],
            dst_ref=est.at[z],
            send_sem=e_send.at[d],
            recv_sem=e_recv.at[d],
            device_id=chan_peer(d),
            device_id_type=MESH,
        )

    def u_copy(d):
        part = pl.ds(pl.multiple_of(lax.rem(z + d, nc) * cz, cz), cz)
        return pltpu.make_async_remote_copy(
            src_ref=ust_send.at[part],
            dst_ref=ust.at[z],
            send_sem=u_send.at[d],
            recv_sem=u_recv.at[d],
            device_id=chan_peer(d),
            device_id_type=MESH,
        )

    for d in far_first:
        e_copy(d).start()
    ust_send[...] = (hidden * own_present).astype(jnp.bfloat16)
    ust[z] = ust_send[own_rows, :]
    for d in far_first:
        u_copy(d).start()
    for d in range(1, nc):
        e_copy(d).wait_recv()
    group = est[0]
    for s in range(1, nc):
        group = group + est[s]
    atoms = zero_row
    for b in range(OWN):
        atoms = atoms + counts[b].astype(jnp.float32)
    plane[g] = jnp.where(lane < OWN * rows, atoms, group)

    def plane_copy(d):
        return pltpu.make_async_remote_copy(
            src_ref=plane.at[g],
            dst_ref=plane.at[g],
            send_sem=plane_sem.at[0],
            recv_sem=plane_sem.at[1],
            device_id=(lax.rem(g + d, na), z),
            device_id_type=MESH,
        )

    if ny > 1:
        pl.semaphore_wait(ready, ny - 1)

    def tell(n, _):
        plane_copy(lax.rem(n + (3 * na) // 8, na - 1) + 1).start()
        return 0

    lax.fori_loop(0, na - 1, tell, 0)
    energies = []
    for b in range(OWN):
        line = jnp.concatenate(
            [est[s, 0:1, rows * b : rows * (b + 1)] for s in range(nc)], axis=1
        )
        energies.append(line * boxes[b][3:4, :])
    energies = jnp.concatenate(energies, axis=0)
    for d in range(1, nc):
        u_copy(d).wait_recv()
    for b in range(OWN):
        upd_out[:, pl.ds(BLK * b, BLK)] = jnp.concatenate(
            [ust[s].astype(jnp.float32)[:, rows * b : rows * (b + 1)] for s in range(nc)], axis=1
        ).astype(jnp.bfloat16)
    others = pltpu.make_async_remote_copy(
        src_ref=plane.at[pl.ds(0, na - 1)],
        dst_ref=plane.at[pl.ds(0, na - 1)],
        send_sem=plane_sem.at[0],
        recv_sem=plane_sem.at[1],
        device_id=(right, z),
        device_id_type=MESH,
    )
    others.wait_recv()
    whole = jnp.sum(plane[:, 0, :], axis=0, keepdims=True)
    scale = jnp.sqrt(1.0 + whole[:, BLK - 1 : BLK] / whole[:, 0:1])
    energy_out[...] = energies / scale
    scale_out[...] = jnp.broadcast_to(scale, (1, BLK))

    for side in range(2):
        meta_copy(side).wait_send()
        for d in range(nc):
            halo_copy(side, d).wait_send()
    for d in range(1, nc):
        feat_copy(d).wait_send()
        w_copy(d).wait_send()
        e_copy(d).wait_send()
        u_copy(d).wait_send()
    others.wait_send()


def per_device(
    na, nc, features, positions, block_counts, radial_w, mix_w, read_w, ghost_lists, tile_pairs, tile_count
):
    cz, width = features.shape
    rows = BLK // nc
    tiles = tile_pairs.shape[1]
    radial_w = radial_w.transpose(1, 0, 2)
    tile_pairs = tile_pairs.transpose(0, 2, 1)
    f32, bf16, i32 = jnp.float32, jnp.bfloat16, jnp.int32
    vm, sm, dma = pltpu.VMEM, pltpu.SMEM, pltpu.SemaphoreType.DMA
    hbm = pl.BlockSpec(memory_space=pltpu.HBM)
    vmem = pl.BlockSpec(memory_space=pltpu.VMEM)
    features, positions, block_counts, radial_w, mix_w, read_w, ghost_lists, tile_pairs = (
        pltpu.with_memory_space_constraint(v, pltpu.HBM)
        for v in (features, positions, block_counts, radial_w, mix_w, read_w, ghost_lists, tile_pairs)
    )
    updated, energies, scale = pl.pallas_call(
        functools.partial(kernel, na, nc),
        out_shape=(
            jax.ShapeDtypeStruct((cz, width), bf16),
            jax.ShapeDtypeStruct((OWN, BLK), f32),
            jax.ShapeDtypeStruct((1, BLK), f32),
        ),
        in_specs=[hbm] * 9,
        out_specs=(vmem, vmem, vmem),
        scratch_shapes=[
            vm((BLK, width), bf16),
            vm((2, BLK, 2 * BLK), bf16),
            vm((3, width), f32),
            vm((4, BLK, BLK), bf16),
            vm((BLK, 4 * BLK), bf16),
            vm((3, NR, cz), f32),
            vm((cz,), f32),
            vm((nc, 8, BLK), f32),
            vm((3, NR, 8, BLK), f32),
            vm((BLK, BLK), f32),
            vm((2, 2, 8, BLK), f32),
            vm((2, 2, 8, BLK), f32),
            vm((2 * OWN, 8, BLK), f32),
            vm((BLK, BLK), f32),
            vm((OWN, 3, rows, BLK), f32),
            vm((2 * OWN, BLK, BLK), bf16),
            vm((PAIRS, NM * NR * rows, 2 * BLK), bf16),
            vm((PAIRS, NM * rows, BLK), f32),
            vm((BLK, BLK), f32),
            vm((BLK, BLK), bf16),
            vm((nc, cz, BLK), bf16),
            vm((nc, 1, BLK), f32),
            vm((na, 1, BLK), f32),
            sm((OWN,), i32),
            sm((1, 2, 2), i32),
            sm((1, 2, tiles), i32),
            sm((1,), i32),
            sm((tiles,), i32),
            sm((2 * PAIRS,), i32),
            sm((2 * PAIRS,), i32),
            sm((PAIRS,), i32),
            sm((OWN,), i32),
            dma((12,)),
            dma((nc,)),
            dma((nc,)),
            dma((nc,)),
            dma((nc,)),
            dma((4,)),
            dma((2, nc)),
            dma((2, nc)),
            dma((nc,)),
            dma((nc,)),
            dma((nc,)),
            dma((nc,)),
            dma((2,)),
            pltpu.SemaphoreType.REGULAR,
        ],
        compiler_params=pltpu.CompilerParams(
            collective_id=0, has_side_effects=True, vmem_limit_bytes=48 * 1024 * 1024
        ),
        name="message_layer",
    )(features, positions, block_counts, radial_w, mix_w, read_w, ghost_lists, tile_pairs, tile_count)
    return updated, energies.reshape(width), scale[0, 0]


def solution(mesh):
    in_specs = (
        P("chan", "atoms"),
        P(None, "atoms"),
        P("atoms"),
        P(None, None, "chan"),
        P(),
        P("chan"),
        P("atoms", None, None),
        P("atoms", None, None),
        P("atoms"),
    )
    out_specs = (P("chan", "atoms"), P("atoms"), P())
    step = functools.partial(per_device, mesh.shape["atoms"], mesh.shape["chan"])
    return jax.shard_map(step, mesh=mesh, in_specs=in_specs, out_specs=out_specs, check_vma=False)
```

```python
import functools

import jax
import jax.numpy as jnp
from jax import lax
from jax.experimental import pallas as pl
from jax.experimental.pallas import tpu as pltpu
from jax.sharding import PartitionSpec as P

MESH = pl.DeviceIdType.MESH
NR = 8
NM = 9
BLK = 128
OWN = 4
PAIRS = 14

root_three = 3.0**0.5
root_fifteen = 15.0**0.5
half_root_five = 0.5 * 5.0**0.5
half_root_fifteen = 0.5 * 15.0**0.5
cutoff_square = 9.0
soften = 0.25
center_step = 3.0 / 7.0
radial_sharp = 2.0
degree = (0, 1, 1, 1, 2, 2, 2, 2, 2)
order = (0, 2, 1, 3)
place_of = (0, 2, 1, 3)


def kernel(
    na,
    nc,
    feat_hbm,
    pos_hbm,
    counts_hbm,
    radial_hbm,
    mix_hbm,
    read_hbm,
    ghost_hbm,
    pairs_hbm,
    live_hbm,
    upd_out,
    energy_out,
    scale_out,
    feat,
    halo,
    pos,
    mixv,
    mixt,
    rw,
    rd,
    wst,
    wb,
    readcol,
    meta,
    meta_in,
    spos,
    tmat,
    rpos,
    sendt,
    kt,
    run,
    fown,
    ust_send,
    ust,
    est,
    plane,
    counts,
    ghost,
    pairs,
    live_count,
    tile_place,
    slot_tile,
    slot_live,
    keep,
    last_slot,
    local_sem,
    feat_sem,
    w_sem,
    meta_sem,
    halo_sem,
    u_sem,
    e_sem,
    plane_sem,
    ready,
):
    cz = feat_hbm.shape[0]
    tiles = pairs.shape[2]
    rows = BLK // nc
    ny = max(1, min(8, na // 2))
    nx = na // (2 * ny)

    g = lax.axis_index("atoms")
    z = lax.axis_index("chan")

    def wrap(v, n):
        return jnp.where(v >= n, v - n, v)

    left, right = wrap(g + na - 1, na), wrap(g + 1, na)
    ci = lax.rem(g, 2)
    yi = lax.rem(lax.div(g, 2), ny)
    xi = lax.div(g, 2 * ny)

    def chan_peer(d):
        return (g, wrap(z + d, nc))

    def y_peer(d):
        return (xi * (2 * ny) + wrap(yi + d, ny) * 2 + ci, z)

    xc = xi * 2 + ci

    def x_peer(d):
        other = wrap(xc + d, 2 * nx)
        return (lax.div(other, 2) * (2 * ny) + yi * 2 + lax.rem(other, 2), z)

    def hail(sem, device):
        pl.semaphore_signal(sem, inc=1, device_id=device, device_id_type=MESH)

    def remote(ref, sems, device=None, to=None):
        return pltpu.make_async_remote_copy(
            src_ref=ref,
            dst_ref=ref if to is None else to,
            send_sem=sems.at[0],
            recv_sem=sems.at[1],
            device_id=chan_peer(1) if device is None else device,
            device_id_type=MESH,
        )

    own_rows = pl.ds(pl.multiple_of(z * cz, cz), cz)

    pos_copy = pltpu.make_async_copy(pos_hbm, pos, local_sem.at[1])
    rw_copy = pltpu.make_async_copy(radial_hbm, rw, local_sem.at[2])
    rd_copy = pltpu.make_async_copy(read_hbm, rd, local_sem.at[3])
    mix_copy = pltpu.make_async_copy(mix_hbm, mixv, local_sem.at[4])
    ints = [
        pltpu.make_async_copy(src, dst, local_sem.at[5 + n])
        for n, (src, dst) in enumerate(
            ((counts_hbm, counts), (ghost_hbm, ghost), (pairs_hbm, pairs), (live_hbm, live_count))
        )
    ]

    for c in ints:
        c.start()
    pos_copy.start()
    for n, b in enumerate(order):
        pltpu.make_async_copy(
            feat_hbm.at[:, pl.ds(BLK * b, BLK)],
            feat.at[own_rows, pl.ds(BLK * n, BLK)],
            local_sem.at[0],
        ).start()
    barrier = pltpu.get_barrier_semaphore()
    far_first = sorted(range(1, nc), key=lambda d: -min(d, nc - d))
    near = [chan_peer(d) for d in far_first] + [(left, z), (right, z)]
    near += [y_peer(d) for d in range(1, ny)]
    near += [x_peer(d) for d in range(1, 2 * nx)]
    for device in near:
        hail(barrier, device)
    rw_copy.start()
    rd_copy.start()
    mix_copy.start()

    def feat_copy(d):
        return pltpu.make_async_remote_copy(
            src_ref=feat.at[own_rows],
            dst_ref=feat.at[own_rows],
            send_sem=feat_sem.at[0],
            recv_sem=feat_sem.at[min(d, nc - d)],
            device_id=chan_peer(d),
            device_id_type=MESH,
        )

    def feat_wait(level, rows_in):
        pltpu.make_async_remote_copy(
            src_ref=feat.at[pl.ds(0, rows_in)],
            dst_ref=feat.at[pl.ds(0, rows_in)],
            send_sem=feat_sem.at[0],
            recv_sem=feat_sem.at[level],
            device_id=chan_peer(1),
            device_id_type=MESH,
        ).wait_recv()

    def pass_on(d):
        part = pl.ds(pl.multiple_of(wrap(z + d, nc) * cz, cz), cz)
        for side in range(2):
            remote(
                feat.at[part, pl.ds(2 * BLK * side, 2 * BLK)],
                halo_sem,
                (left if side == 0 else right, z),
                halo.at[1 - side, part],
            ).start()

    lane = lax.broadcasted_iota(jnp.int32, (1, BLK), 1)
    for c in ints:
        c.wait()
    pos_copy.wait()
    zero_row = jnp.zeros((1, BLK), jnp.float32)
    boxes = []
    for b in range(OWN):
        where = pos[:, pl.ds(BLK * b, BLK)]
        present = (lane < counts[b]).astype(jnp.float32)
        low = (ghost[0, 0, 0] >> 1).astype(jnp.float32)
        high = (ghost[0, 1, 0] >> 1).astype(jnp.float32)
        rows8 = jnp.concatenate(
            [where, present, zero_row + low, zero_row + high, zero_row, zero_row], axis=0
        )
        boxes.append(rows8)
        spos[b] = rows8
    swap_low = ghost[0, 0, 0] != 0
    swap_high = ghost[0, 1, 0] != 1
    meta[0, 0] = jnp.where(swap_low, boxes[2], boxes[0])
    meta[0, 1] = jnp.where(swap_low, boxes[0], boxes[2])
    meta[1, 0] = jnp.where(swap_high, boxes[3], boxes[1])
    meta[1, 1] = jnp.where(swap_high, boxes[1], boxes[3])

    rw_copy.wait()
    rd_copy.wait()
    folded = jnp.concatenate([rw[:, k, :] for k in range(NR)], axis=1)
    read_row = jnp.concatenate(
        [rd[...].reshape(1, cz), jnp.zeros((1, BLK - cz), jnp.float32)], axis=1
    )
    wst[z] = jnp.concatenate([folded, read_row], axis=0)

    total = live_count[0]

    sizes = [jnp.int32(0)] * OWN
    ranks = []
    for t in range(tiles):
        r = pairs[0, 0, t]
        alive = (t < total).astype(jnp.int32)
        rank = sizes[0]
        for b in range(1, OWN):
            rank = jnp.where(r == b, sizes[b], rank)
        ranks.append(rank)
        sizes = [n + jnp.where(r == b, alive, 0) for b, n in enumerate(sizes)]
    starts = [jnp.int32(0)]
    for b in range(OWN):
        used = (sizes[b] + 1) >> 1
        last_slot[b] = jnp.maximum(starts[b] + used - 1, 0)
        starts.append(starts[b] + used)
    for t in range(tiles):
        r = pairs[0, 0, t]
        first = starts[0]
        for b in range(1, OWN):
            first = jnp.where(r == b, starts[b], first)
        tile_place[t] = jnp.where(t < total, 2 * first + ranks[t], -1)

    for p in range(PAIRS):
        same = jnp.int32(1)
        for b in range(OWN):
            same = jnp.where(starts[b] == p, 0, same)
        keep[p] = same

    def fill(n, _):
        found = [jnp.int32(0)] * 4
        for t in range(tiles):
            place = tile_place[t]
            found = [jnp.where(place == 4 * n + u, t + 32, f) for u, f in enumerate(found)]
        for u, f in enumerate(found):
            slot_tile[4 * n + u] = f & 31
            slot_live[4 * n + u] = f >> 5
        return 0

    lax.fori_loop(0, PAIRS // 2, fill, 0)

    pltpu.make_async_copy(feat_hbm, feat.at[own_rows], local_sem.at[0]).wait()
    pl.semaphore_wait(barrier, len(near))
    for side in range(2):
        remote(
            meta.at[side], meta_sem, (left if side == 0 else right, z), meta_in.at[1 - side]
        ).start()
    for d in far_first:
        feat_copy(d).start()
        remote(wst.at[z], w_sem, chan_peer(d)).start()
    pass_on(0)
    for d in range(1, ny):
        hail(ready, y_peer(d))

    tmat[...] = jnp.zeros((BLK, BLK), jnp.float32)
    for b in range(OWN):
        tmat[pl.ds(8 * b, 8), :] = boxes[b]
    tmat[...] = tmat[...].T
    mine = tmat[pl.ds(pl.multiple_of(z * rows, rows), rows), :]
    for b in range(OWN):
        for d in range(3):
            rpos[b, d] = jnp.broadcast_to(mine[:, 8 * b + d : 8 * b + d + 1], (rows, BLK))

    remote(meta, meta_sem).wait_recv()
    for side in range(2):
        for n in range(2):
            spos[OWN + 2 * side + n] = meta_in[side, n]

    shape = (rows, BLK)
    own_index = lax.broadcasted_iota(jnp.int32, shape, 0) + z * rows
    off_diagonal = (own_index != lax.broadcasted_iota(jnp.int32, shape, 1)).astype(jnp.float32)

    def geometry(p, half):
        s = 2 * p + half
        t = slot_tile[s]
        r = pairs[0, 0, t]
        q = pairs[0, 1, t]
        there = spos[q]
        weight = slot_live[s].astype(jnp.float32)
        own = (q == r).astype(jnp.float32)
        off = [there[d : d + 1, :] - rpos[r, d] for d in range(3)]
        dist_sq = off[0] * off[0] + off[1] * off[1] + off[2] * off[2]
        shut = jnp.square(jnp.maximum(1.0 - dist_sq / cutoff_square, 0.0))
        shut = shut * (1.0 - own * (1.0 - off_diagonal))
        shut = shut * (there[3:4, :] * weight)
        distance = jnp.sqrt(dist_sq + soften)
        inverse = 1.0 / distance
        ux, uy, uz = (o * inverse for o in off)
        angular = (
            None,
            root_three * ux,
            root_three * uy,
            root_three * uz,
            root_fifteen * ux * uy,
            root_fifteen * uy * uz,
            half_root_five * (2.0 * uz * uz - ux * ux - uy * uy),
            root_fifteen * ux * uz,
            half_root_fifteen * (ux * ux - uy * uy),
        )
        angular = [shut if y is None else y * shut for y in angular]
        for k in range(NR):
            radial = jnp.exp(-radial_sharp * jnp.square(distance - k * center_step))
            for m in range(NM):
                kt[p, pl.ds((m * NR + k) * rows, rows), pl.ds(BLK * half, BLK)] = (
                    radial * angular[m]
                ).astype(jnp.bfloat16)

    def two_pairs(n, _):
        for u in range(2):
            for half in range(2):
                geometry(2 * n + u, half)
        return 0

    lax.fori_loop(0, PAIRS // 2, two_pairs, 0)
    for d in range(1, nc // 2):
        feat_wait(d, 2 * cz)
        pass_on(d)
        pass_on(nc - d)
    feat_wait(nc // 2, cz)
    pass_on(nc // 2)

    for b in range(OWN):
        sendt[b] = feat[:, pl.ds(BLK * place_of[b], BLK)].T
    shift = lax.rem(BLK - z * rows, BLK)
    fown[...] = jnp.concatenate(
        [
            pltpu.roll(feat[:, pl.ds(BLK * place_of[b], BLK)].astype(jnp.float32), shift, 1)[:, :rows]
            for b in range(OWN)
        ]
        + [jnp.zeros((BLK, BLK - OWN * rows), jnp.float32)],
        axis=1,
    )
    own_present = jnp.concatenate(
        [pltpu.roll(boxes[b], shift, 1)[3:4, :rows] for b in range(OWN)]
        + [jnp.zeros((1, BLK - OWN * rows), jnp.float32)],
        axis=1,
    )
    mix_copy.wait()
    for n in range(4):
        mixt[:, pl.ds(BLK * n, BLK)] = mixv[n].T
    remote(wst.at[pl.ds(0, nc - 1)], w_sem).wait_recv()
    for k in range(NR):
        whole = jnp.concatenate([wst[s, :, cz * k : cz * (k + 1)] for s in range(nc)], axis=1)
        for l in range(3):
            wb[l, k] = jnp.broadcast_to(whole[l : l + 1, :], (8, BLK))
        if k == 0:
            readcol[...] = jnp.broadcast_to(whole[3:4, :], (BLK, BLK)).T
    remote(halo, halo_sem).wait_recv()
    for side in range(2):
        bit = meta_in[side, 0][5 - side : 6 - side, :] > 0.5
        early = halo[side, :, 0:BLK].astype(jnp.float32)
        late = halo[side, :, BLK : 2 * BLK].astype(jnp.float32)
        sendt[OWN + 2 * side] = jnp.where(bit, late, early).astype(jnp.bfloat16).T
        sendt[OWN + 2 * side + 1] = jnp.where(bit, early, late).astype(jnp.bfloat16).T

    def message(p):
        q0 = pairs[0, 1, slot_tile[2 * p]]
        q1 = pairs[0, 1, slot_tile[2 * p + 1]]
        both = jnp.concatenate([sendt[q0], sendt[q1]], axis=0)
        kept = keep[p].astype(jnp.float32)
        part = jnp.dot(kt[p], both, preferred_element_type=jnp.float32)
        for m in range(NM):
            acc = 0.0 if p == 0 else run[p - 1, pl.ds(m * rows, rows), :] * kept
            for k in range(NR):
                w = wb[degree[m], k]
                at = (m * NR + k) * rows
                acc = acc + jnp.concatenate([w] * (rows // 8), axis=0) * part[at : at + rows, :]
            run[p, pl.ds(m * rows, rows), :] = acc

    for p in range(PAIRS):
        message(p)

    basis = []
    for b in range(OWN):
        slot = last_slot[b]
        den = [run[slot, pl.ds(m * rows, rows), :] for m in range(NM)]
        vec = den[1] * den[1] + den[2] * den[2] + den[3] * den[3]
        ten = sum(den[m] * den[m] for m in range(5, NM)) + den[4] * den[4]
        basis.append(jnp.concatenate([den[0], den[0] * den[0], vec, ten], axis=1))
    basis = jnp.concatenate(
        basis + [jnp.zeros((BLK - OWN * rows, 4 * BLK), jnp.float32)], axis=0
    ).astype(jnp.bfloat16)
    mixed = lax.dot_general(
        mixt[...], basis, (((1,), (1,)), ((), ())), preferred_element_type=jnp.float32
    )
    hidden = fown[...] + mixed / (1.0 + jnp.exp(-mixed))
    energy = jnp.sum(readcol[...] * hidden, axis=0, keepdims=True)
    square = jnp.sum(energy * energy * own_present, axis=1, keepdims=True)
    est[z] = jnp.where(lane < OWN * rows, energy, jnp.broadcast_to(square, (1, BLK)))

    for d in far_first:
        remote(est.at[z], e_sem, chan_peer(d)).start()
    ust_send[...] = (hidden * own_present).astype(jnp.bfloat16)
    ust[z] = ust_send[own_rows, :]
    for d in far_first:
        part = pl.ds(pl.multiple_of(wrap(z + d, nc) * cz, cz), cz)
        remote(ust_send.at[part], u_sem, chan_peer(d), ust.at[z]).start()
    remote(est.at[pl.ds(0, nc - 1)], e_sem).wait_recv()
    group = est[0]
    for s in range(1, nc):
        group = group + est[s]
    atoms = zero_row
    for b in range(OWN):
        atoms = atoms + counts[b].astype(jnp.float32)
    plane[g] = jnp.where(lane < OWN * rows, atoms, group)

    if ny > 1:
        pl.semaphore_wait(ready, ny - 1)
    for n in range(na - 1):
        d = (n + (3 * na) // 8) % (na - 1) + 1
        remote(plane.at[g], plane_sem, (wrap(g + d, na), z)).start()
    energies = []
    for b in range(OWN):
        line = jnp.concatenate(
            [est[s, 0:1, rows * b : rows * (b + 1)] for s in range(nc)], axis=1
        )
        energies.append(line * boxes[b][3:4, :])
    energies = jnp.concatenate(energies, axis=0)
    remote(ust.at[pl.ds(0, nc - 1)], u_sem).wait_recv()
    for b in range(OWN):
        upd_out[:, pl.ds(BLK * b, BLK)] = jnp.concatenate(
            [ust[s].astype(jnp.float32)[:, rows * b : rows * (b + 1)] for s in range(nc)], axis=1
        ).astype(jnp.bfloat16)
    others = remote(plane.at[pl.ds(0, na - 1)], plane_sem)
    others.wait_recv()
    whole = jnp.sum(plane[:, 0, :], axis=0, keepdims=True)
    scale = jnp.sqrt(1.0 + whole[:, BLK - 1 : BLK] / whole[:, 0:1])
    energy_out[...] = energies / scale
    scale_out[...] = jnp.broadcast_to(scale, (1, BLK))

    remote(meta, meta_sem).wait_send()
    remote(halo, halo_sem).wait_send()
    remote(feat.at[pl.ds(0, (nc - 1) * cz)], feat_sem).wait_send()
    remote(wst.at[pl.ds(0, nc - 1)], w_sem).wait_send()
    remote(est.at[pl.ds(0, nc - 1)], e_sem).wait_send()
    remote(ust.at[pl.ds(0, nc - 1)], u_sem).wait_send()
    others.wait_send()


def per_device(
    na, nc, features, positions, block_counts, radial_w, mix_w, read_w, ghost_lists, tile_pairs, tile_count
):
    cz, width = features.shape
    rows = BLK // nc
    tiles = tile_pairs.shape[1]
    radial_w = radial_w.transpose(1, 0, 2)
    tile_pairs = tile_pairs.transpose(0, 2, 1)
    f32, bf16, i32 = jnp.float32, jnp.bfloat16, jnp.int32
    vm, sm, dma = pltpu.VMEM, pltpu.SMEM, pltpu.SemaphoreType.DMA
    hbm = pl.BlockSpec(memory_space=pltpu.HBM)
    vmem = pl.BlockSpec(memory_space=pltpu.VMEM)
    features, positions, block_counts, radial_w, mix_w, read_w, ghost_lists, tile_pairs = (
        pltpu.with_memory_space_constraint(v, pltpu.HBM)
        for v in (features, positions, block_counts, radial_w, mix_w, read_w, ghost_lists, tile_pairs)
    )
    updated, energies, scale = pl.pallas_call(
        functools.partial(kernel, na, nc),
        out_shape=(
            jax.ShapeDtypeStruct((cz, width), bf16),
            jax.ShapeDtypeStruct((OWN, BLK), f32),
            jax.ShapeDtypeStruct((1, BLK), f32),
        ),
        in_specs=[hbm] * 9,
        out_specs=(vmem, vmem, vmem),
        scratch_shapes=[
            vm((BLK, width), bf16),
            vm((2, BLK, 2 * BLK), bf16),
            vm((3, width), f32),
            vm((4, BLK, BLK), bf16),
            vm((BLK, 4 * BLK), bf16),
            vm((3, NR, cz), f32),
            vm((cz,), f32),
            vm((nc, 4, BLK), f32),
            vm((3, NR, 8, BLK), f32),
            vm((BLK, BLK), f32),
            vm((2, 2, 8, BLK), f32),
            vm((2, 2, 8, BLK), f32),
            vm((2 * OWN, 8, BLK), f32),
            vm((BLK, BLK), f32),
            vm((OWN, 3, rows, BLK), f32),
            vm((2 * OWN, BLK, BLK), bf16),
            vm((PAIRS, NM * NR * rows, 2 * BLK), bf16),
            vm((PAIRS, NM * rows, BLK), f32),
            vm((BLK, BLK), f32),
            vm((BLK, BLK), bf16),
            vm((nc, cz, BLK), bf16),
            vm((nc, 1, BLK), f32),
            vm((na, 1, BLK), f32),
            sm((OWN,), i32),
            sm((1, 2, 2), i32),
            sm((1, 2, tiles), i32),
            sm((1,), i32),
            sm((tiles,), i32),
            sm((2 * PAIRS,), i32),
            sm((2 * PAIRS,), i32),
            sm((PAIRS,), i32),
            sm((OWN,), i32),
            dma((9,)),
            dma((5,)),
            dma((2,)),
            dma((2,)),
            dma((2,)),
            dma((2,)),
            dma((2,)),
            dma((2,)),
            pltpu.SemaphoreType.REGULAR,
        ],
        compiler_params=pltpu.CompilerParams(
            collective_id=0, has_side_effects=True, vmem_limit_bytes=48 * 1024 * 1024
        ),
        name="message_layer",
    )(features, positions, block_counts, radial_w, mix_w, read_w, ghost_lists, tile_pairs, tile_count)
    return updated, energies.reshape(width), scale[0, 0]


def solution(mesh):
    in_specs = (
        P("chan", "atoms"),
        P(None, "atoms"),
        P("atoms"),
        P(None, None, "chan"),
        P(),
        P("chan"),
        P("atoms", None, None),
        P("atoms", None, None),
        P("atoms"),
    )
    out_specs = (P("chan", "atoms"), P("atoms"), P())
    step = functools.partial(per_device, mesh.shape["atoms"], mesh.shape["chan"])
    return jax.shard_map(step, mesh=mesh, in_specs=in_specs, out_specs=out_specs, check_vma=False)
```

```python
import functools

import jax
import jax.numpy as jnp
from jax import lax
from jax.experimental import pallas as pl
from jax.experimental.pallas import tpu as pltpu
from jax.sharding import PartitionSpec as P

MESH = pl.DeviceIdType.MESH
NR = 8
NM = 9
BLK = 128
OWN = 4
PAIRS = 14

root_three = 3.0**0.5
root_fifteen = 15.0**0.5
half_root_five = 0.5 * 5.0**0.5
half_root_fifteen = 0.5 * 15.0**0.5
cutoff_square = 9.0
soften = 0.25
center_step = 3.0 / 7.0
radial_sharp = 2.0
degree = (0, 1, 1, 1, 2, 2, 2, 2, 2)
order = (0, 2, 1, 3)
place_of = (0, 2, 1, 3)


def kernel(
    na,
    nc,
    feat_hbm,
    pos_hbm,
    counts_hbm,
    radial_hbm,
    mix_hbm,
    read_hbm,
    ghost_hbm,
    pairs_hbm,
    live_hbm,
    upd_out,
    energy_out,
    scale_out,
    feat,
    halo,
    pos,
    mixv,
    mixt,
    rw,
    rd,
    wst,
    wb,
    readcol,
    meta,
    meta_in,
    spos,
    tmat,
    rpos,
    sendt,
    kt,
    run,
    fown,
    ust_send,
    ust,
    est,
    plane,
    counts,
    ghost,
    pairs,
    live_count,
    tile_place,
    slot_tile,
    slot_live,
    keep,
    last_slot,
    local_sem,
    feat_sem,
    w_sem,
    meta_sem,
    halo_sem,
    u_sem,
    e_sem,
    plane_sem,
    ready,
):
    cz = feat_hbm.shape[0]
    tiles = pairs.shape[2]
    rows = BLK // nc
    ny = max(1, min(8, na // 2))
    nx = na // (2 * ny)

    g = lax.axis_index("atoms")
    z = lax.axis_index("chan")

    def wrap(v, n):
        return jnp.where(v >= n, v - n, v)

    left, right = wrap(g + na - 1, na), wrap(g + 1, na)
    ci = lax.rem(g, 2)
    yi = lax.rem(lax.div(g, 2), ny)
    xi = lax.div(g, 2 * ny)

    def chan_peer(d):
        return (g, wrap(z + d, nc))

    def y_peer(d):
        return (xi * (2 * ny) + wrap(yi + d, ny) * 2 + ci, z)

    xc = xi * 2 + ci

    def x_peer(d):
        other = wrap(xc + d, 2 * nx)
        return (lax.div(other, 2) * (2 * ny) + yi * 2 + lax.rem(other, 2), z)

    def hail(sem, device):
        pl.semaphore_signal(sem, inc=1, device_id=device, device_id_type=MESH)

    def remote(ref, sems, device=None, to=None):
        return pltpu.make_async_remote_copy(
            src_ref=ref,
            dst_ref=ref if to is None else to,
            send_sem=sems.at[0],
            recv_sem=sems.at[1],
            device_id=chan_peer(1) if device is None else device,
            device_id_type=MESH,
        )

    own_rows = pl.ds(pl.multiple_of(z * cz, cz), cz)

    pos_copy = pltpu.make_async_copy(pos_hbm, pos, local_sem.at[1])
    rw_copy = pltpu.make_async_copy(radial_hbm, rw, local_sem.at[2])
    rd_copy = pltpu.make_async_copy(read_hbm, rd, local_sem.at[3])
    mix_copy = pltpu.make_async_copy(mix_hbm, mixv, local_sem.at[4])
    ints = [
        pltpu.make_async_copy(src, dst, local_sem.at[5 + n])
        for n, (src, dst) in enumerate(
            ((counts_hbm, counts), (ghost_hbm, ghost), (pairs_hbm, pairs), (live_hbm, live_count))
        )
    ]

    for c in ints:
        c.start()
    pos_copy.start()
    for n, b in enumerate(order):
        pltpu.make_async_copy(
            feat_hbm.at[:, pl.ds(BLK * b, BLK)],
            feat.at[own_rows, pl.ds(BLK * n, BLK)],
            local_sem.at[0],
        ).start()
    barrier = pltpu.get_barrier_semaphore()
    far_first = sorted(range(1, nc), key=lambda d: -min(d, nc - d))
    near = [chan_peer(d) for d in far_first] + [(left, z), (right, z)]
    near += [y_peer(d) for d in range(1, ny)]
    near += [x_peer(d) for d in range(1, 2 * nx)]
    for device in near:
        hail(barrier, device)
    rw_copy.start()
    rd_copy.start()
    mix_copy.start()

    def feat_copy(d):
        return pltpu.make_async_remote_copy(
            src_ref=feat.at[own_rows],
            dst_ref=feat.at[own_rows],
            send_sem=feat_sem.at[0],
            recv_sem=feat_sem.at[min(d, nc - d)],
            device_id=chan_peer(d),
            device_id_type=MESH,
        )

    def feat_wait(level, rows_in):
        pltpu.make_async_remote_copy(
            src_ref=feat.at[pl.ds(0, rows_in)],
            dst_ref=feat.at[pl.ds(0, rows_in)],
            send_sem=feat_sem.at[0],
            recv_sem=feat_sem.at[level],
            device_id=chan_peer(1),
            device_id_type=MESH,
        ).wait_recv()

    def pass_on(d):
        part = pl.ds(pl.multiple_of(wrap(z + d, nc) * cz, cz), cz)
        for side in range(2):
            remote(
                feat.at[part, pl.ds(2 * BLK * side, 2 * BLK)],
                halo_sem,
                (left if side == 0 else right, z),
                halo.at[1 - side, part],
            ).start()

    lane = lax.broadcasted_iota(jnp.int32, (1, BLK), 1)
    for c in ints:
        c.wait()
    pos_copy.wait()
    zero_row = jnp.zeros((1, BLK), jnp.float32)
    boxes = []
    for b in range(OWN):
        where = pos[:, pl.ds(BLK * b, BLK)]
        present = (lane < counts[b]).astype(jnp.float32)
        low = (ghost[0, 0, 0] >> 1).astype(jnp.float32)
        high = (ghost[0, 1, 0] >> 1).astype(jnp.float32)
        rows8 = jnp.concatenate(
            [where, present, zero_row + low, zero_row + high, zero_row, zero_row], axis=0
        )
        boxes.append(rows8)
        spos[b] = rows8
    swap_low = ghost[0, 0, 0] != 0
    swap_high = ghost[0, 1, 0] != 1
    meta[0, 0] = jnp.where(swap_low, boxes[2], boxes[0])
    meta[0, 1] = jnp.where(swap_low, boxes[0], boxes[2])
    meta[1, 0] = jnp.where(swap_high, boxes[3], boxes[1])
    meta[1, 1] = jnp.where(swap_high, boxes[1], boxes[3])

    rw_copy.wait()
    rd_copy.wait()
    folded = jnp.concatenate([rw[:, k, :] for k in range(NR)], axis=1)
    read_row = jnp.concatenate(
        [rd[...].reshape(1, cz), jnp.zeros((1, BLK - cz), jnp.float32)], axis=1
    )
    wst[z] = jnp.concatenate([folded, read_row], axis=0)

    total = live_count[0]

    sizes = [jnp.int32(0)] * OWN
    ranks = []
    for t in range(tiles):
        r = pairs[0, 0, t]
        alive = (t < total).astype(jnp.int32)
        rank = sizes[0]
        for b in range(1, OWN):
            rank = jnp.where(r == b, sizes[b], rank)
        ranks.append(rank)
        sizes = [n + jnp.where(r == b, alive, 0) for b, n in enumerate(sizes)]
    starts = [jnp.int32(0)]
    for b in range(OWN):
        used = (sizes[b] + 1) >> 1
        last_slot[b] = jnp.maximum(starts[b] + used - 1, 0)
        starts.append(starts[b] + used)
    for t in range(tiles):
        r = pairs[0, 0, t]
        first = starts[0]
        for b in range(1, OWN):
            first = jnp.where(r == b, starts[b], first)
        tile_place[t] = jnp.where(t < total, 2 * first + ranks[t], -1)

    for p in range(PAIRS):
        same = jnp.int32(1)
        for b in range(OWN):
            same = jnp.where(starts[b] == p, 0, same)
        keep[p] = same

    def fill(n, _):
        found = [jnp.int32(0)] * 4
        for t in range(tiles):
            place = tile_place[t]
            found = [jnp.where(place == 4 * n + u, t + 32, f) for u, f in enumerate(found)]
        for u, f in enumerate(found):
            slot_tile[4 * n + u] = f & 31
            slot_live[4 * n + u] = f >> 5
        return 0

    lax.fori_loop(0, PAIRS // 2, fill, 0)

    pltpu.make_async_copy(feat_hbm, feat.at[own_rows], local_sem.at[0]).wait()
    pl.semaphore_wait(barrier, len(near))
    for side in range(2):
        remote(
            meta.at[side], meta_sem, (left if side == 0 else right, z), meta_in.at[1 - side]
        ).start()
    for d in far_first:
        feat_copy(d).start()
        remote(wst.at[z], w_sem, chan_peer(d)).start()
    pass_on(0)
    for d in range(1, ny):
        hail(ready, y_peer(d))

    tmat[...] = jnp.zeros((BLK, BLK), jnp.float32)
    for b in range(OWN):
        tmat[pl.ds(8 * b, 8), :] = boxes[b]
    tmat[...] = tmat[...].T
    mine = tmat[pl.ds(pl.multiple_of(z * rows, rows), rows), :]
    for b in range(OWN):
        for d in range(3):
            rpos[b, d] = jnp.broadcast_to(mine[:, 8 * b + d : 8 * b + d + 1], (rows, BLK))

    remote(meta, meta_sem).wait_recv()
    for side in range(2):
        for n in range(2):
            spos[OWN + 2 * side + n] = meta_in[side, n]

    shape = (rows, BLK)
    own_index = lax.broadcasted_iota(jnp.int32, shape, 0) + z * rows
    off_diagonal = (own_index != lax.broadcasted_iota(jnp.int32, shape, 1)).astype(jnp.float32)

    def geometry(p, half):
        s = 2 * p + half
        t = slot_tile[s]
        r = pairs[0, 0, t]
        q = pairs[0, 1, t]
        there = spos[q]
        weight = slot_live[s].astype(jnp.float32)
        own = (q == r).astype(jnp.float32)
        off = [there[d : d + 1, :] - rpos[r, d] for d in range(3)]
        dist_sq = off[0] * off[0] + off[1] * off[1] + off[2] * off[2]
        shut = jnp.square(jnp.maximum(1.0 - dist_sq / cutoff_square, 0.0))
        shut = shut * (1.0 - own * (1.0 - off_diagonal))
        shut = shut * (there[3:4, :] * weight)
        distance = jnp.sqrt(dist_sq + soften)
        inverse = 1.0 / distance
        ux, uy, uz = (o * inverse for o in off)
        angular = (
            None,
            root_three * ux,
            root_three * uy,
            root_three * uz,
            root_fifteen * ux * uy,
            root_fifteen * uy * uz,
            half_root_five * (2.0 * uz * uz - ux * ux - uy * uy),
            root_fifteen * ux * uz,
            half_root_fifteen * (ux * ux - uy * uy),
        )
        angular = [shut if y is None else y * shut for y in angular]
        for k in range(NR):
            radial = jnp.exp(-radial_sharp * jnp.square(distance - k * center_step))
            for m in range(NM):
                kt[p, pl.ds((m * NR + k) * rows, rows), pl.ds(BLK * half, BLK)] = (
                    radial * angular[m]
                ).astype(jnp.bfloat16)

    def two_pairs(n, _):
        for u in range(2):
            for half in range(2):
                geometry(2 * n + u, half)
        return 0

    lax.fori_loop(0, PAIRS // 2, two_pairs, 0)
    for d in range(1, nc // 2):
        feat_wait(d, 2 * cz)
        pass_on(d)
        pass_on(nc - d)
    feat_wait(nc // 2, cz)
    pass_on(nc // 2)

    for b in range(OWN):
        sendt[b] = feat[:, pl.ds(BLK * place_of[b], BLK)].T
    shift = lax.rem(BLK - z * rows, BLK)
    fown[...] = jnp.concatenate(
        [
            pltpu.roll(feat[:, pl.ds(BLK * place_of[b], BLK)].astype(jnp.float32), shift, 1)[:, :rows]
            for b in range(OWN)
        ]
        + [jnp.zeros((BLK, BLK - OWN * rows), jnp.float32)],
        axis=1,
    )
    own_present = jnp.concatenate(
        [pltpu.roll(boxes[b], shift, 1)[3:4, :rows] for b in range(OWN)]
        + [jnp.zeros((1, BLK - OWN * rows), jnp.float32)],
        axis=1,
    )
    mix_copy.wait()
    for n in range(4):
        mixt[:, pl.ds(BLK * n, BLK)] = mixv[n].T
    remote(wst.at[pl.ds(0, nc - 1)], w_sem).wait_recv()
    for k in range(NR):
        whole = jnp.concatenate([wst[s, :, cz * k : cz * (k + 1)] for s in range(nc)], axis=1)
        for l in range(3):
            wb[l, k] = jnp.broadcast_to(whole[l : l + 1, :], (8, BLK))
        if k == 0:
            readcol[...] = jnp.broadcast_to(whole[3:4, :], (BLK, BLK)).T
    remote(halo, halo_sem).wait_recv()
    for side in range(2):
        bit = meta_in[side, 0][5 - side : 6 - side, :] > 0.5
        early = halo[side, :, 0:BLK].astype(jnp.float32)
        late = halo[side, :, BLK : 2 * BLK].astype(jnp.float32)
        sendt[OWN + 2 * side] = jnp.where(bit, late, early).astype(jnp.bfloat16).T
        sendt[OWN + 2 * side + 1] = jnp.where(bit, early, late).astype(jnp.bfloat16).T

    def message(p):
        q0 = pairs[0, 1, slot_tile[2 * p]]
        q1 = pairs[0, 1, slot_tile[2 * p + 1]]
        both = jnp.concatenate([sendt[q0], sendt[q1]], axis=0)
        kept = keep[p].astype(jnp.float32)
        part = jnp.dot(kt[p], both, preferred_element_type=jnp.float32)
        for m in range(NM):
            acc = 0.0 if p == 0 else run[p - 1, pl.ds(m * rows, rows), :] * kept
            for k in range(NR):
                w = wb[degree[m], k]
                at = (m * NR + k) * rows
                acc = acc + jnp.concatenate([w] * (rows // 8), axis=0) * part[at : at + rows, :]
            run[p, pl.ds(m * rows, rows), :] = acc

    for p in range(PAIRS):
        message(p)

    basis = []
    for b in range(OWN):
        slot = last_slot[b]
        den = [run[slot, pl.ds(m * rows, rows), :] for m in range(NM)]
        vec = den[1] * den[1] + den[2] * den[2] + den[3] * den[3]
        ten = sum(den[m] * den[m] for m in range(5, NM)) + den[4] * den[4]
        basis.append(jnp.concatenate([den[0], den[0] * den[0], vec, ten], axis=1))
    basis = jnp.concatenate(
        basis + [jnp.zeros((BLK - OWN * rows, 4 * BLK), jnp.float32)], axis=0
    ).astype(jnp.bfloat16)
    mixed = lax.dot_general(
        mixt[...], basis, (((1,), (1,)), ((), ())), preferred_element_type=jnp.float32
    )
    hidden = fown[...] + mixed / (1.0 + jnp.exp(-mixed))
    energy = jnp.sum(readcol[...] * hidden, axis=0, keepdims=True)
    square = jnp.sum(energy * energy * own_present, axis=1, keepdims=True)
    est[z] = jnp.where(lane < OWN * rows, energy, jnp.broadcast_to(square, (1, BLK)))

    for d in far_first:
        remote(est.at[z], e_sem, chan_peer(d)).start()
    ust_send[...] = (hidden * own_present).astype(jnp.bfloat16)
    ust[z] = ust_send[own_rows, :]
    for d in far_first:
        part = pl.ds(pl.multiple_of(wrap(z + d, nc) * cz, cz), cz)
        remote(ust_send.at[part], u_sem, chan_peer(d), ust.at[z]).start()
    remote(est.at[pl.ds(0, nc - 1)], e_sem).wait_recv()
    group = est[0]
    for s in range(1, nc):
        group = group + est[s]
    atoms = zero_row
    for b in range(OWN):
        atoms = atoms + counts[b].astype(jnp.float32)
    plane[g] = jnp.where(lane < OWN * rows, atoms, group)

    if ny > 1:
        pl.semaphore_wait(ready, ny - 1)
    for n in range(na - 1):
        d = (n + (3 * na) // 8) % (na - 1) + 1
        remote(plane.at[g], plane_sem, (wrap(g + d, na), z)).start()
    energies = []
    for b in range(OWN):
        line = jnp.concatenate(
            [est[s, 0:1, rows * b : rows * (b + 1)] for s in range(nc)], axis=1
        )
        energies.append(line * boxes[b][3:4, :])
    energies = jnp.concatenate(energies, axis=0)
    remote(ust.at[pl.ds(0, nc - 1)], u_sem).wait_recv()
    for b in range(OWN):
        upd_out[:, pl.ds(BLK * b, BLK)] = jnp.concatenate(
            [ust[s].astype(jnp.float32)[:, rows * b : rows * (b + 1)] for s in range(nc)], axis=1
        ).astype(jnp.bfloat16)
    others = remote(plane.at[pl.ds(0, na - 1)], plane_sem)
    others.wait_recv()
    whole = jnp.sum(plane[:, 0, :], axis=0, keepdims=True)
    scale = jnp.sqrt(1.0 + whole[:, BLK - 1 : BLK] / whole[:, 0:1])
    energy_out[...] = energies / scale
    scale_out[...] = jnp.broadcast_to(scale, (1, BLK))

    remote(meta, meta_sem).wait_send()
    remote(halo, halo_sem).wait_send()
    remote(feat.at[pl.ds(0, (nc - 1) * cz)], feat_sem).wait_send()
    remote(wst.at[pl.ds(0, nc - 1)], w_sem).wait_send()
    remote(est.at[pl.ds(0, nc - 1)], e_sem).wait_send()
    remote(ust.at[pl.ds(0, nc - 1)], u_sem).wait_send()
    others.wait_send()


def settle(updated, energies, scale, updated_out, energies_out, scale_out, sems):
    copies = [
        pltpu.make_async_copy(src, dst, sems.at[n])
        for n, (src, dst) in enumerate(
            ((updated, updated_out), (energies, energies_out), (scale, scale_out))
        )
    ]
    for c in copies:
        c.start()
    for c in copies:
        c.wait()


def per_device(
    na, nc, features, positions, block_counts, radial_w, mix_w, read_w, ghost_lists, tile_pairs, tile_count
):
    cz, width = features.shape
    rows = BLK // nc
    tiles = tile_pairs.shape[1]
    radial_w = radial_w.transpose(1, 0, 2)
    tile_pairs = tile_pairs.transpose(0, 2, 1)
    f32, bf16, i32 = jnp.float32, jnp.bfloat16, jnp.int32
    vm, sm, dma = pltpu.VMEM, pltpu.SMEM, pltpu.SemaphoreType.DMA
    hbm = pl.BlockSpec(memory_space=pltpu.HBM)
    vmem = pl.BlockSpec(memory_space=pltpu.VMEM)
    features, positions, block_counts, radial_w, mix_w, read_w, ghost_lists, tile_pairs = (
        pltpu.with_memory_space_constraint(v, pltpu.HBM)
        for v in (features, positions, block_counts, radial_w, mix_w, read_w, ghost_lists, tile_pairs)
    )
    updated, energies, scale = pl.pallas_call(
        functools.partial(kernel, na, nc),
        out_shape=(
            jax.ShapeDtypeStruct((cz, width), bf16),
            jax.ShapeDtypeStruct((OWN, BLK), f32),
            jax.ShapeDtypeStruct((1, BLK), f32),
        ),
        in_specs=[hbm] * 9,
        out_specs=(vmem, vmem, vmem),
        scratch_shapes=[
            vm((BLK, width), bf16),
            vm((2, BLK, 2 * BLK), bf16),
            vm((3, width), f32),
            vm((4, BLK, BLK), bf16),
            vm((BLK, 4 * BLK), bf16),
            vm((3, NR, cz), f32),
            vm((cz,), f32),
            vm((nc, 4, BLK), f32),
            vm((3, NR, 8, BLK), f32),
            vm((BLK, BLK), f32),
            vm((2, 2, 8, BLK), f32),
            vm((2, 2, 8, BLK), f32),
            vm((2 * OWN, 8, BLK), f32),
            vm((BLK, BLK), f32),
            vm((OWN, 3, rows, BLK), f32),
            vm((2 * OWN, BLK, BLK), bf16),
            vm((PAIRS, NM * NR * rows, 2 * BLK), bf16),
            vm((PAIRS, NM * rows, BLK), f32),
            vm((BLK, BLK), f32),
            vm((BLK, BLK), bf16),
            vm((nc, cz, BLK), bf16),
            vm((nc, 1, BLK), f32),
            vm((na, 1, BLK), f32),
            sm((OWN,), i32),
            sm((1, 2, 2), i32),
            sm((1, 2, tiles), i32),
            sm((1,), i32),
            sm((tiles,), i32),
            sm((2 * PAIRS,), i32),
            sm((2 * PAIRS,), i32),
            sm((PAIRS,), i32),
            sm((OWN,), i32),
            dma((9,)),
            dma((5,)),
            dma((2,)),
            dma((2,)),
            dma((2,)),
            dma((2,)),
            dma((2,)),
            dma((2,)),
            pltpu.SemaphoreType.REGULAR,
        ],
        compiler_params=pltpu.CompilerParams(
            collective_id=0, has_side_effects=True, vmem_limit_bytes=48 * 1024 * 1024
        ),
        name="message_layer",
    )(features, positions, block_counts, radial_w, mix_w, read_w, ghost_lists, tile_pairs, tile_count)
    updated, energies, scale = pl.pallas_call(
        settle,
        out_shape=(
            jax.ShapeDtypeStruct((cz, width), bf16),
            jax.ShapeDtypeStruct((OWN, BLK), f32),
            jax.ShapeDtypeStruct((1, BLK), f32),
        ),
        in_specs=[pl.BlockSpec(memory_space=pl.ANY)] * 3,
        out_specs=(hbm, hbm, hbm),
        scratch_shapes=[dma((3,))],
        compiler_params=pltpu.CompilerParams(vmem_limit_bytes=1024 * 1024),
        name="settle",
    )(updated, energies, scale)
    return updated, energies.reshape(width), scale[0, 0]


def solution(mesh):
    in_specs = (
        P("chan", "atoms"),
        P(None, "atoms"),
        P("atoms"),
        P(None, None, "chan"),
        P(),
        P("chan"),
        P("atoms", None, None),
        P("atoms", None, None),
        P("atoms"),
    )
    out_specs = (P("chan", "atoms"), P("atoms"), P())
    step = functools.partial(per_device, mesh.shape["atoms"], mesh.shape["chan"])
    return jax.shard_map(step, mesh=mesh, in_specs=in_specs, out_specs=out_specs, check_vma=False)
```

```python
import functools

import jax
import jax.numpy as jnp
from jax import lax
from jax.experimental import pallas as pl
from jax.experimental.pallas import tpu as pltpu
from jax.sharding import PartitionSpec as P

MESH = pl.DeviceIdType.MESH
NR = 8
NM = 9
BLK = 128
OWN = 4
PAIRS = 14

root_three = 3.0**0.5
root_fifteen = 15.0**0.5
half_root_five = 0.5 * 5.0**0.5
half_root_fifteen = 0.5 * 15.0**0.5
cutoff_square = 9.0
soften = 0.25
center_step = 3.0 / 7.0
radial_sharp = 2.0
degree = (0, 1, 1, 1, 2, 2, 2, 2, 2)
order = (0, 2, 1, 3)
place_of = (0, 2, 1, 3)


def kernel(
    na,
    nc,
    feat_hbm,
    pos_hbm,
    counts_hbm,
    radial_hbm,
    mix_hbm,
    read_hbm,
    ghost_hbm,
    pairs_hbm,
    live_hbm,
    upd_out,
    energy_out,
    scale_out,
    feat,
    halo,
    pos,
    mixv,
    mixt,
    rw,
    rd,
    wst,
    wb,
    readcol,
    meta,
    meta_in,
    spos,
    tmat,
    rpos,
    sendt,
    kt,
    run,
    fown,
    ust_send,
    ust,
    est,
    plane,
    counts,
    ghost,
    pairs,
    live_count,
    tile_place,
    slot_tile,
    slot_live,
    keep,
    last_slot,
    feat_sem,
    w_sem,
    meta_sem,
    halo_sem,
    u_sem,
    e_sem,
    plane_sem,
    ready,
    local_sem,
):
    cz = feat_hbm.shape[0]
    tiles = pairs.shape[2]
    rows = BLK // nc
    ny = max(1, min(8, na // 2))
    nx = na // (2 * ny)

    g = lax.axis_index("atoms")
    z = lax.axis_index("chan")

    def wrap(v, n):
        return jnp.where(v >= n, v - n, v)

    left, right = wrap(g + na - 1, na), wrap(g + 1, na)
    ci = lax.rem(g, 2)
    yi = lax.rem(lax.div(g, 2), ny)
    xi = lax.div(g, 2 * ny)

    def chan_peer(d):
        return (g, wrap(z + d, nc))

    def y_peer(d):
        return (xi * (2 * ny) + wrap(yi + d, ny) * 2 + ci, z)

    xc = xi * 2 + ci

    def x_peer(d):
        other = wrap(xc + d, 2 * nx)
        return (lax.div(other, 2) * (2 * ny) + yi * 2 + lax.rem(other, 2), z)

    def hail(sem, device):
        pl.semaphore_signal(sem, inc=1, device_id=device, device_id_type=MESH)

    def remote(ref, sems, device=None, to=None):
        return pltpu.make_async_remote_copy(
            src_ref=ref,
            dst_ref=ref if to is None else to,
            send_sem=feat_sem.at[0] if sems.shape[0] == 1 else sems.at[0],
            recv_sem=sems.at[sems.shape[0] - 1],
            device_id=chan_peer(1) if device is None else device,
            device_id_type=MESH,
        )

    own_rows = pl.ds(pl.multiple_of(z * cz, cz), cz)

    pos_copy = pltpu.make_async_copy(pos_hbm, pos, local_sem.at[1])
    rw_copy = pltpu.make_async_copy(radial_hbm, rw, local_sem.at[2])
    rd_copy = pltpu.make_async_copy(read_hbm, rd, local_sem.at[3])
    mix_copy = pltpu.make_async_copy(mix_hbm, mixv, local_sem.at[4])
    ints = [
        pltpu.make_async_copy(src, dst, local_sem.at[5 + n])
        for n, (src, dst) in enumerate(
            ((counts_hbm, counts), (ghost_hbm, ghost), (pairs_hbm, pairs), (live_hbm, live_count))
        )
    ]

    for c in ints:
        c.start()
    pos_copy.start()
    for n, b in enumerate(order):
        pltpu.make_async_copy(
            feat_hbm.at[:, pl.ds(BLK * b, BLK)],
            feat.at[own_rows, pl.ds(BLK * n, BLK)],
            local_sem.at[0],
        ).start()
    barrier = pltpu.get_barrier_semaphore()
    far_first = sorted(range(1, nc), key=lambda d: -min(d, nc - d))
    near = [chan_peer(d) for d in far_first] + [(left, z), (right, z)]
    near += [y_peer(d) for d in range(1, ny)]
    near += [x_peer(d) for d in range(1, 2 * nx)]
    for device in near:
        hail(barrier, device)
    rw_copy.start()
    rd_copy.start()
    mix_copy.start()

    def feat_copy(d):
        return pltpu.make_async_remote_copy(
            src_ref=feat.at[own_rows],
            dst_ref=feat.at[own_rows],
            send_sem=feat_sem.at[0],
            recv_sem=feat_sem.at[min(d, nc - d)],
            device_id=chan_peer(d),
            device_id_type=MESH,
        )

    def feat_wait(level, rows_in):
        pltpu.make_async_remote_copy(
            src_ref=feat.at[pl.ds(0, rows_in)],
            dst_ref=feat.at[pl.ds(0, rows_in)],
            send_sem=feat_sem.at[0],
            recv_sem=feat_sem.at[level],
            device_id=chan_peer(1),
            device_id_type=MESH,
        ).wait_recv()

    def pass_on(d):
        part = pl.ds(pl.multiple_of(wrap(z + d, nc) * cz, cz), cz)
        for side in range(2):
            remote(
                feat.at[part, pl.ds(2 * BLK * side, 2 * BLK)],
                halo_sem,
                (left if side == 0 else right, z),
                halo.at[1 - side, part],
            ).start()

    lane = lax.broadcasted_iota(jnp.int32, (1, BLK), 1)
    for c in ints:
        c.wait()
    pos_copy.wait()
    zero_row = jnp.zeros((1, BLK), jnp.float32)
    boxes = []
    for b in range(OWN):
        where = pos[:, pl.ds(BLK * b, BLK)]
        present = (lane < counts[b]).astype(jnp.float32)
        low = (ghost[0, 0, 0] >> 1).astype(jnp.float32)
        high = (ghost[0, 1, 0] >> 1).astype(jnp.float32)
        rows8 = jnp.concatenate(
            [where, present, zero_row + low, zero_row + high, zero_row, zero_row], axis=0
        )
        boxes.append(rows8)
        spos[b] = rows8
    swap_low = ghost[0, 0, 0] != 0
    swap_high = ghost[0, 1, 0] != 1
    meta[0, 0] = jnp.where(swap_low, boxes[2], boxes[0])
    meta[0, 1] = jnp.where(swap_low, boxes[0], boxes[2])
    meta[1, 0] = jnp.where(swap_high, boxes[3], boxes[1])
    meta[1, 1] = jnp.where(swap_high, boxes[1], boxes[3])

    rw_copy.wait()
    rd_copy.wait()
    folded = jnp.concatenate([rw[:, k, :] for k in range(NR)], axis=1)
    read_row = jnp.concatenate(
        [rd[...].reshape(1, cz), jnp.zeros((1, BLK - cz), jnp.float32)], axis=1
    )
    wst[z] = jnp.concatenate([folded, read_row], axis=0)

    total = live_count[0]

    sizes = [jnp.int32(0)] * OWN
    ranks = []
    for t in range(tiles):
        r = pairs[0, 0, t]
        alive = (t < total).astype(jnp.int32)
        rank = sizes[0]
        for b in range(1, OWN):
            rank = jnp.where(r == b, sizes[b], rank)
        ranks.append(rank)
        sizes = [n + jnp.where(r == b, alive, 0) for b, n in enumerate(sizes)]
    starts = [jnp.int32(0)]
    for b in range(OWN):
        used = (sizes[b] + 1) >> 1
        last_slot[b] = jnp.maximum(starts[b] + used - 1, 0)
        starts.append(starts[b] + used)
    for t in range(tiles):
        r = pairs[0, 0, t]
        first = starts[0]
        for b in range(1, OWN):
            first = jnp.where(r == b, starts[b], first)
        tile_place[t] = jnp.where(t < total, 2 * first + ranks[t], -1)

    for p in range(PAIRS):
        same = jnp.int32(1)
        for b in range(OWN):
            same = jnp.where(starts[b] == p, 0, same)
        keep[p] = same

    def fill(n, _):
        found = [jnp.int32(0)] * 4
        for t in range(tiles):
            place = tile_place[t]
            found = [jnp.where(place == 4 * n + u, t + 32, f) for u, f in enumerate(found)]
        for u, f in enumerate(found):
            slot_tile[4 * n + u] = f & 31
            slot_live[4 * n + u] = f >> 5
        return 0

    lax.fori_loop(0, PAIRS // 2, fill, 0)

    pltpu.make_async_copy(feat_hbm, feat.at[own_rows], local_sem.at[0]).wait()
    pl.semaphore_wait(barrier, len(near))
    for side in range(2):
        remote(
            meta.at[side], meta_sem, (left if side == 0 else right, z), meta_in.at[1 - side]
        ).start()
    for d in far_first:
        feat_copy(d).start()
        remote(wst.at[z], w_sem, chan_peer(d)).start()
    pass_on(0)
    for d in range(1, ny):
        hail(ready, y_peer(d))

    tmat[...] = jnp.zeros((BLK, BLK), jnp.float32)
    for b in range(OWN):
        tmat[pl.ds(8 * b, 8), :] = boxes[b]
    tmat[...] = tmat[...].T
    mine = tmat[pl.ds(pl.multiple_of(z * rows, rows), rows), :]
    for b in range(OWN):
        for d in range(3):
            rpos[b, d] = jnp.broadcast_to(mine[:, 8 * b + d : 8 * b + d + 1], (rows, BLK))

    remote(meta, meta_sem).wait_recv()
    for side in range(2):
        for n in range(2):
            spos[OWN + 2 * side + n] = meta_in[side, n]

    shape = (rows, BLK)
    own_index = lax.broadcasted_iota(jnp.int32, shape, 0) + z * rows
    off_diagonal = (own_index != lax.broadcasted_iota(jnp.int32, shape, 1)).astype(jnp.float32)

    def geometry(p, half):
        s = 2 * p + half
        t = slot_tile[s]
        r = pairs[0, 0, t]
        q = pairs[0, 1, t]
        there = spos[q]
        weight = slot_live[s].astype(jnp.float32)
        own = (q == r).astype(jnp.float32)
        off = [there[d : d + 1, :] - rpos[r, d] for d in range(3)]
        dist_sq = off[0] * off[0] + off[1] * off[1] + off[2] * off[2]
        shut = jnp.square(jnp.maximum(1.0 - dist_sq / cutoff_square, 0.0))
        shut = shut * (1.0 - own * (1.0 - off_diagonal))
        shut = shut * (there[3:4, :] * weight)
        distance = jnp.sqrt(dist_sq + soften)
        inverse = 1.0 / distance
        ux, uy, uz = (o * inverse for o in off)
        angular = (
            None,
            root_three * ux,
            root_three * uy,
            root_three * uz,
            root_fifteen * ux * uy,
            root_fifteen * uy * uz,
            half_root_five * (2.0 * uz * uz - ux * ux - uy * uy),
            root_fifteen * ux * uz,
            half_root_fifteen * (ux * ux - uy * uy),
        )
        angular = [shut if y is None else y * shut for y in angular]
        for k in range(NR):
            radial = jnp.exp(-radial_sharp * jnp.square(distance - k * center_step))
            for m in range(NM):
                kt[p, pl.ds((m * NR + k) * rows, rows), pl.ds(BLK * half, BLK)] = (
                    radial * angular[m]
                ).astype(jnp.bfloat16)

    def two_pairs(n, _):
        for u in range(2):
            for half in range(2):
                geometry(2 * n + u, half)
        return 0

    lax.fori_loop(0, PAIRS // 2, two_pairs, 0)
    for d in range(1, nc // 2):
        feat_wait(d, 2 * cz)
        pass_on(d)
        pass_on(nc - d)
    feat_wait(nc // 2, cz)
    pass_on(nc // 2)

    for b in range(OWN):
        sendt[b] = feat[:, pl.ds(BLK * place_of[b], BLK)].T
    shift = lax.rem(BLK - z * rows, BLK)
    fown[...] = jnp.concatenate(
        [
            pltpu.roll(feat[:, pl.ds(BLK * place_of[b], BLK)].astype(jnp.float32), shift, 1)[:, :rows]
            for b in range(OWN)
        ]
        + [jnp.zeros((BLK, BLK - OWN * rows), jnp.float32)],
        axis=1,
    )
    own_present = jnp.concatenate(
        [pltpu.roll(boxes[b], shift, 1)[3:4, :rows] for b in range(OWN)]
        + [jnp.zeros((1, BLK - OWN * rows), jnp.float32)],
        axis=1,
    )
    mix_copy.wait()
    for n in range(4):
        mixt[:, pl.ds(BLK * n, BLK)] = mixv[n].T
    remote(wst.at[pl.ds(0, nc - 1)], w_sem).wait_recv()
    for k in range(NR):
        whole = jnp.concatenate([wst[s, :, cz * k : cz * (k + 1)] for s in range(nc)], axis=1)
        for l in range(3):
            wb[l, k] = jnp.broadcast_to(whole[l : l + 1, :], (8, BLK))
        if k == 0:
            readcol[...] = jnp.broadcast_to(whole[3:4, :], (BLK, BLK)).T
    remote(halo, halo_sem).wait_recv()
    for side in range(2):
        bit = meta_in[side, 0][5 - side : 6 - side, :] > 0.5
        early = halo[side, :, 0:BLK].astype(jnp.float32)
        late = halo[side, :, BLK : 2 * BLK].astype(jnp.float32)
        sendt[OWN + 2 * side] = jnp.where(bit, late, early).astype(jnp.bfloat16).T
        sendt[OWN + 2 * side + 1] = jnp.where(bit, early, late).astype(jnp.bfloat16).T

    def message(p):
        q0 = pairs[0, 1, slot_tile[2 * p]]
        q1 = pairs[0, 1, slot_tile[2 * p + 1]]
        both = jnp.concatenate([sendt[q0], sendt[q1]], axis=0)
        kept = keep[p].astype(jnp.float32)
        part = jnp.dot(kt[p], both, preferred_element_type=jnp.float32)
        for m in range(NM):
            acc = 0.0 if p == 0 else run[p - 1, pl.ds(m * rows, rows), :] * kept
            for k in range(NR):
                w = wb[degree[m], k]
                at = (m * NR + k) * rows
                acc = acc + jnp.concatenate([w] * (rows // 8), axis=0) * part[at : at + rows, :]
            run[p, pl.ds(m * rows, rows), :] = acc

    for p in range(PAIRS):
        message(p)

    basis = []
    for b in range(OWN):
        slot = last_slot[b]
        den = [run[slot, pl.ds(m * rows, rows), :] for m in range(NM)]
        vec = den[1] * den[1] + den[2] * den[2] + den[3] * den[3]
        ten = sum(den[m] * den[m] for m in range(5, NM)) + den[4] * den[4]
        basis.append(jnp.concatenate([den[0], den[0] * den[0], vec, ten], axis=1))
    basis = jnp.concatenate(
        basis + [jnp.zeros((BLK - OWN * rows, 4 * BLK), jnp.float32)], axis=0
    ).astype(jnp.bfloat16)
    mixed = lax.dot_general(
        mixt[...], basis, (((1,), (1,)), ((), ())), preferred_element_type=jnp.float32
    )
    hidden = fown[...] + mixed / (1.0 + jnp.exp(-mixed))
    energy = jnp.sum(readcol[...] * hidden, axis=0, keepdims=True)
    square = jnp.sum(energy * energy * own_present, axis=1, keepdims=True)
    est[z] = jnp.where(lane < OWN * rows, energy, jnp.broadcast_to(square, (1, BLK)))

    for d in far_first:
        remote(est.at[z], e_sem, chan_peer(d)).start()
    ust_send[...] = (hidden * own_present).astype(jnp.bfloat16)
    ust[z] = ust_send[own_rows, :]
    for d in far_first:
        part = pl.ds(pl.multiple_of(wrap(z + d, nc) * cz, cz), cz)
        remote(ust_send.at[part], u_sem, chan_peer(d), ust.at[z]).start()
    remote(est.at[pl.ds(0, nc - 1)], e_sem).wait_recv()
    group = est[0]
    for s in range(1, nc):
        group = group + est[s]
    atoms = zero_row
    for b in range(OWN):
        atoms = atoms + counts[b].astype(jnp.float32)
    plane[g] = jnp.where(lane < OWN * rows, atoms, group)

    if ny > 1:
        pl.semaphore_wait(ready, ny - 1)
    for n in range(na - 1):
        d = (n + (3 * na) // 8) % (na - 1) + 1
        remote(plane.at[g], plane_sem, (wrap(g + d, na), z)).start()
    energies = []
    for b in range(OWN):
        line = jnp.concatenate(
            [est[s, 0:1, rows * b : rows * (b + 1)] for s in range(nc)], axis=1
        )
        energies.append(line * boxes[b][3:4, :])
    energies = jnp.concatenate(energies, axis=0)
    remote(ust.at[pl.ds(0, nc - 1)], u_sem).wait_recv()
    for b in range(OWN):
        upd_out[:, pl.ds(BLK * b, BLK)] = jnp.concatenate(
            [ust[s].astype(jnp.float32)[:, rows * b : rows * (b + 1)] for s in range(nc)], axis=1
        ).astype(jnp.bfloat16)
    others = remote(plane.at[pl.ds(0, na - 1)], plane_sem)
    others.wait_recv()
    whole = jnp.sum(plane[:, 0, :], axis=0, keepdims=True)
    scale = jnp.sqrt(1.0 + whole[:, BLK - 1 : BLK] / whole[:, 0:1])
    energy_out[...] = energies / scale
    scale_out[...] = jnp.broadcast_to(scale, (1, BLK))

    remote(kt.at[0, pl.ds(0, 32 * nc * 2)], halo_sem).wait_send()
    remote(wst.at[pl.ds(0, nc - 1)], w_sem).wait_send()
    remote(est.at[pl.ds(0, nc - 1)], e_sem).wait_send()
    remote(ust.at[pl.ds(0, nc - 1)], u_sem).wait_send()
    others.wait_send()


def scoped(na, nc, *refs):
    pl.run_scoped(lambda sem: kernel(na, nc, *refs, sem), pltpu.SemaphoreType.DMA((9,)))


def settle(updated, energies, scale, updated_out, energies_out, scale_out, sems):
    copies = [
        pltpu.make_async_copy(src, dst, sems.at[n])
        for n, (src, dst) in enumerate(
            ((updated, updated_out), (energies, energies_out), (scale, scale_out))
        )
    ]
    for c in copies:
        c.start()
    for c in copies:
        c.wait()


def per_device(
    na, nc, features, positions, block_counts, radial_w, mix_w, read_w, ghost_lists, tile_pairs, tile_count
):
    cz, width = features.shape
    rows = BLK // nc
    tiles = tile_pairs.shape[1]
    radial_w = radial_w.transpose(1, 0, 2)
    tile_pairs = tile_pairs.transpose(0, 2, 1)
    f32, bf16, i32 = jnp.float32, jnp.bfloat16, jnp.int32
    vm, sm, dma = pltpu.VMEM, pltpu.SMEM, pltpu.SemaphoreType.DMA
    hbm = pl.BlockSpec(memory_space=pltpu.HBM)
    vmem = pl.BlockSpec(memory_space=pltpu.VMEM)
    features, positions, block_counts, radial_w, mix_w, read_w, ghost_lists, tile_pairs = (
        pltpu.with_memory_space_constraint(v, pltpu.HBM)
        for v in (features, positions, block_counts, radial_w, mix_w, read_w, ghost_lists, tile_pairs)
    )
    updated, energies, scale = pl.pallas_call(
        functools.partial(scoped, na, nc),
        out_shape=(
            jax.ShapeDtypeStruct((cz, width), bf16),
            jax.ShapeDtypeStruct((OWN, BLK), f32),
            jax.ShapeDtypeStruct((1, BLK), f32),
        ),
        in_specs=[hbm] * 9,
        out_specs=(vmem, vmem, vmem),
        scratch_shapes=[
            vm((BLK, width), bf16),
            vm((2, BLK, 2 * BLK), bf16),
            vm((3, width), f32),
            vm((4, BLK, BLK), bf16),
            vm((BLK, 4 * BLK), bf16),
            vm((3, NR, cz), f32),
            vm((cz,), f32),
            vm((nc, 4, BLK), f32),
            vm((3, NR, 8, BLK), f32),
            vm((BLK, BLK), f32),
            vm((2, 2, 8, BLK), f32),
            vm((2, 2, 8, BLK), f32),
            vm((2 * OWN, 8, BLK), f32),
            vm((BLK, BLK), f32),
            vm((OWN, 3, rows, BLK), f32),
            vm((2 * OWN, BLK, BLK), bf16),
            vm((PAIRS, NM * NR * rows, 2 * BLK), bf16),
            vm((PAIRS, NM * rows, BLK), f32),
            vm((BLK, BLK), f32),
            vm((BLK, BLK), bf16),
            vm((nc, cz, BLK), bf16),
            vm((nc, 1, BLK), f32),
            vm((na, 1, BLK), f32),
            sm((OWN,), i32),
            sm((1, 2, 2), i32),
            sm((1, 2, tiles), i32),
            sm((1,), i32),
            sm((tiles,), i32),
            sm((2 * PAIRS,), i32),
            sm((2 * PAIRS,), i32),
            sm((PAIRS,), i32),
            sm((OWN,), i32),
            dma((5,)),
            dma((2,)),
            dma((1,)),
            dma((1,)),
            dma((2,)),
            dma((2,)),
            dma((2,)),
            pltpu.SemaphoreType.REGULAR,
        ],
        compiler_params=pltpu.CompilerParams(
            collective_id=0, has_side_effects=True, vmem_limit_bytes=48 * 1024 * 1024
        ),
        name="message_layer",
    )(features, positions, block_counts, radial_w, mix_w, read_w, ghost_lists, tile_pairs, tile_count)
    updated, energies, scale = pl.pallas_call(
        settle,
        out_shape=(
            jax.ShapeDtypeStruct((cz, width), bf16),
            jax.ShapeDtypeStruct((OWN, BLK), f32),
            jax.ShapeDtypeStruct((1, BLK), f32),
        ),
        in_specs=[pl.BlockSpec(memory_space=pl.ANY)] * 3,
        out_specs=(hbm, hbm, hbm),
        scratch_shapes=[dma((3,))],
        compiler_params=pltpu.CompilerParams(vmem_limit_bytes=1024 * 1024),
        name="settle",
    )(updated, energies, scale)
    return updated, energies.reshape(width), scale[0, 0]


def solution(mesh):
    in_specs = (
        P("chan", "atoms"),
        P(None, "atoms"),
        P("atoms"),
        P(None, None, "chan"),
        P(),
        P("chan"),
        P("atoms", None, None),
        P("atoms", None, None),
        P("atoms"),
    )
    out_specs = (P("chan", "atoms"), P("atoms"), P())
    step = functools.partial(per_device, mesh.shape["atoms"], mesh.shape["chan"])
    return jax.shard_map(step, mesh=mesh, in_specs=in_specs, out_specs=out_specs, check_vma=False)
```

```python
import functools

import jax
import jax.numpy as jnp
from jax import lax
from jax.experimental import pallas as pl
from jax.experimental.pallas import tpu as pltpu
from jax.sharding import PartitionSpec as P

MESH = pl.DeviceIdType.MESH
NR = 8
NM = 9
BLK = 128
OWN = 4
PAIRS = 14

root_three = 3.0**0.5
root_fifteen = 15.0**0.5
half_root_five = 0.5 * 5.0**0.5
half_root_fifteen = 0.5 * 15.0**0.5
cutoff_square = 9.0
soften = 0.25
center_step = 3.0 / 7.0
radial_sharp = 2.0
degree = (0, 1, 1, 1, 2, 2, 2, 2, 2)
order = (0, 2, 1, 3)
place_of = (0, 2, 1, 3)


def kernel(
    na,
    nc,
    feat_hbm,
    pos_hbm,
    counts_hbm,
    radial_hbm,
    mix_hbm,
    read_hbm,
    ghost_hbm,
    pairs_hbm,
    live_hbm,
    upd_out,
    energy_out,
    scale_out,
    feat,
    halo,
    pos,
    mixv,
    mixt,
    rw,
    rd,
    wst,
    wb,
    readcol,
    meta,
    meta_in,
    spos,
    tmat,
    rpos,
    sendt,
    kt,
    run,
    fown,
    ust_send,
    ust,
    est,
    plane,
    counts,
    ghost,
    pairs,
    live_count,
    tile_place,
    slot_tile,
    slot_live,
    keep,
    last_slot,
    feat_sem,
    w_sem,
    meta_sem,
    halo_sem,
    u_sem,
    e_sem,
    plane_sem,
    ready,
    local_sem,
):
    cz = feat_hbm.shape[0]
    tiles = pairs.shape[2]
    rows = BLK // nc
    ny = max(1, min(8, na // 2))
    nx = na // (2 * ny)

    g = lax.axis_index("atoms")
    z = lax.axis_index("chan")

    def wrap(v, n):
        return jnp.where(v >= n, v - n, v)

    left, right = wrap(g + na - 1, na), wrap(g + 1, na)
    ci = lax.rem(g, 2)
    yi = lax.rem(lax.div(g, 2), ny)
    xi = lax.div(g, 2 * ny)

    def chan_peer(d):
        return (g, wrap(z + d, nc))

    def y_peer(d):
        return (xi * (2 * ny) + wrap(yi + d, ny) * 2 + ci, z)

    xc = xi * 2 + ci

    def x_peer(d):
        other = wrap(xc + d, 2 * nx)
        return (lax.div(other, 2) * (2 * ny) + yi * 2 + lax.rem(other, 2), z)

    def hail(sem, device):
        pl.semaphore_signal(sem, inc=1, device_id=device, device_id_type=MESH)

    def remote(ref, sems, device=None, to=None):
        return pltpu.make_async_remote_copy(
            src_ref=ref,
            dst_ref=ref if to is None else to,
            send_sem=feat_sem.at[0] if sems.shape[0] == 1 else sems.at[0],
            recv_sem=sems.at[sems.shape[0] - 1],
            device_id=chan_peer(1) if device is None else device,
            device_id_type=MESH,
        )

    own_rows = pl.ds(pl.multiple_of(z * cz, cz), cz)

    pos_copy = pltpu.make_async_copy(pos_hbm, pos, local_sem.at[1])
    rw_copy = pltpu.make_async_copy(radial_hbm, rw, local_sem.at[2])
    rd_copy = pltpu.make_async_copy(read_hbm, rd, local_sem.at[3])
    mix_copy = pltpu.make_async_copy(mix_hbm, mixv, local_sem.at[4])
    ints = [
        pltpu.make_async_copy(src, dst, local_sem.at[5 + n])
        for n, (src, dst) in enumerate(
            ((counts_hbm, counts), (ghost_hbm, ghost), (pairs_hbm, pairs), (live_hbm, live_count))
        )
    ]

    for c in ints:
        c.start()
    pos_copy.start()
    for n, b in enumerate(order):
        pltpu.make_async_copy(
            feat_hbm.at[:, pl.ds(BLK * b, BLK)],
            feat.at[own_rows, pl.ds(BLK * n, BLK)],
            local_sem.at[0],
        ).start()
    barrier = pltpu.get_barrier_semaphore()
    far_first = sorted(range(1, nc), key=lambda d: -min(d, nc - d))
    near = [chan_peer(d) for d in far_first] + [(left, z), (right, z)]
    near += [y_peer(d) for d in range(1, ny)]
    near += [x_peer(d) for d in range(1, 2 * nx)]
    for device in near:
        hail(barrier, device)
    rw_copy.start()
    rd_copy.start()
    mix_copy.start()

    def feat_copy(d):
        return pltpu.make_async_remote_copy(
            src_ref=feat.at[own_rows],
            dst_ref=feat.at[own_rows],
            send_sem=feat_sem.at[0],
            recv_sem=feat_sem.at[min(d, nc - d)],
            device_id=chan_peer(d),
            device_id_type=MESH,
        )

    def feat_wait(level, rows_in):
        pltpu.make_async_remote_copy(
            src_ref=feat.at[pl.ds(0, rows_in)],
            dst_ref=feat.at[pl.ds(0, rows_in)],
            send_sem=feat_sem.at[0],
            recv_sem=feat_sem.at[level],
            device_id=chan_peer(1),
            device_id_type=MESH,
        ).wait_recv()

    def pass_on(d):
        part = pl.ds(pl.multiple_of(wrap(z + d, nc) * cz, cz), cz)
        for side in range(2):
            remote(
                feat.at[part, pl.ds(2 * BLK * side, 2 * BLK)],
                halo_sem,
                (left if side == 0 else right, z),
                halo.at[1 - side, part],
            ).start()

    lane = lax.broadcasted_iota(jnp.int32, (1, BLK), 1)
    for c in ints:
        c.wait()
    pos_copy.wait()
    zero_row = jnp.zeros((1, BLK), jnp.float32)
    boxes = []
    for b in range(OWN):
        where = pos[:, pl.ds(BLK * b, BLK)]
        present = (lane < counts[b]).astype(jnp.float32)
        low = (ghost[0, 0, 0] >> 1).astype(jnp.float32)
        high = (ghost[0, 1, 0] >> 1).astype(jnp.float32)
        rows8 = jnp.concatenate(
            [where, present, zero_row + low, zero_row + high, zero_row, zero_row], axis=0
        )
        boxes.append(rows8)
        spos[b] = rows8
    swap_low = ghost[0, 0, 0] != 0
    swap_high = ghost[0, 1, 0] != 1
    meta[0, 0] = jnp.where(swap_low, boxes[2], boxes[0])
    meta[0, 1] = jnp.where(swap_low, boxes[0], boxes[2])
    meta[1, 0] = jnp.where(swap_high, boxes[3], boxes[1])
    meta[1, 1] = jnp.where(swap_high, boxes[1], boxes[3])

    rw_copy.wait()
    rd_copy.wait()
    folded = jnp.concatenate([rw[:, k, :] for k in range(NR)], axis=1)
    read_row = jnp.concatenate(
        [rd[...].reshape(1, cz), jnp.zeros((1, BLK - cz), jnp.float32)], axis=1
    )
    wst[z] = jnp.concatenate([folded, read_row], axis=0)

    total = live_count[0]

    sizes = [jnp.int32(0)] * OWN
    ranks = []
    for t in range(tiles):
        r = pairs[0, 0, t]
        alive = (t < total).astype(jnp.int32)
        rank = sizes[0]
        for b in range(1, OWN):
            rank = jnp.where(r == b, sizes[b], rank)
        ranks.append(rank)
        sizes = [n + jnp.where(r == b, alive, 0) for b, n in enumerate(sizes)]
    starts = [jnp.int32(0)]
    for b in range(OWN):
        used = (sizes[b] + 1) >> 1
        last_slot[b] = jnp.maximum(starts[b] + used - 1, 0)
        starts.append(starts[b] + used)
    for t in range(tiles):
        r = pairs[0, 0, t]
        first = starts[0]
        for b in range(1, OWN):
            first = jnp.where(r == b, starts[b], first)
        tile_place[t] = jnp.where(t < total, 2 * first + ranks[t], -1)

    for p in range(PAIRS):
        same = jnp.int32(1)
        for b in range(OWN):
            same = jnp.where(starts[b] == p, 0, same)
        keep[p] = same

    def fill(n, _):
        found = [jnp.int32(0)] * 4
        for t in range(tiles):
            place = tile_place[t]
            found = [jnp.where(place == 4 * n + u, t + 32, f) for u, f in enumerate(found)]
        for u, f in enumerate(found):
            slot_tile[4 * n + u] = f & 31
            slot_live[4 * n + u] = f >> 5
        return 0

    lax.fori_loop(0, PAIRS // 2, fill, 0)

    pltpu.make_async_copy(feat_hbm, feat.at[own_rows], local_sem.at[0]).wait()
    pl.semaphore_wait(barrier, len(near))
    for side in range(2):
        remote(
            meta.at[side], meta_sem, (left if side == 0 else right, z), meta_in.at[1 - side]
        ).start()
    for d in far_first:
        feat_copy(d).start()
        remote(wst.at[z], w_sem, chan_peer(d)).start()
    pass_on(0)
    for d in range(1, ny):
        hail(ready, y_peer(d))

    tmat[...] = jnp.zeros((BLK, BLK), jnp.float32)
    for b in range(OWN):
        tmat[pl.ds(8 * b, 8), :] = boxes[b]
    tmat[...] = tmat[...].T
    mine = tmat[pl.ds(pl.multiple_of(z * rows, rows), rows), :]
    for b in range(OWN):
        for d in range(3):
            rpos[b, d] = jnp.broadcast_to(mine[:, 8 * b + d : 8 * b + d + 1], (rows, BLK))

    remote(meta, meta_sem).wait_recv()
    for side in range(2):
        for n in range(2):
            spos[OWN + 2 * side + n] = meta_in[side, n]

    shape = (rows, BLK)
    own_index = lax.broadcasted_iota(jnp.int32, shape, 0) + z * rows
    off_diagonal = (own_index != lax.broadcasted_iota(jnp.int32, shape, 1)).astype(jnp.float32)

    def geometry(p, half):
        s = 2 * p + half
        t = slot_tile[s]
        r = pairs[0, 0, t]
        q = pairs[0, 1, t]
        there = spos[q]
        weight = slot_live[s].astype(jnp.float32)
        own = (q == r).astype(jnp.float32)
        off = [there[d : d + 1, :] - rpos[r, d] for d in range(3)]
        dist_sq = off[0] * off[0] + off[1] * off[1] + off[2] * off[2]
        shut = jnp.square(jnp.maximum(1.0 - dist_sq / cutoff_square, 0.0))
        shut = shut * (1.0 - own * (1.0 - off_diagonal))
        shut = shut * (there[3:4, :] * weight)
        distance = jnp.sqrt(dist_sq + soften)
        inverse = 1.0 / distance
        ux, uy, uz = (o * inverse for o in off)
        angular = (
            None,
            root_three * ux,
            root_three * uy,
            root_three * uz,
            root_fifteen * ux * uy,
            root_fifteen * uy * uz,
            half_root_five * (2.0 * uz * uz - ux * ux - uy * uy),
            root_fifteen * ux * uz,
            half_root_fifteen * (ux * ux - uy * uy),
        )
        angular = [shut if y is None else y * shut for y in angular]
        for k in range(NR):
            radial = jnp.exp(-radial_sharp * jnp.square(distance - k * center_step))
            for m in range(NM):
                kt[p, pl.ds((m * NR + k) * rows, rows), pl.ds(BLK * half, BLK)] = (
                    radial * angular[m]
                ).astype(jnp.bfloat16)

    def two_pairs(n, _):
        for u in range(2):
            for half in range(2):
                geometry(2 * n + u, half)
        return 0

    lax.fori_loop(0, PAIRS // 2, two_pairs, 0)
    for d in range(1, nc // 2):
        feat_wait(d, 2 * cz)
        pass_on(d)
        pass_on(nc - d)
    feat_wait(nc // 2, cz)
    pass_on(nc // 2)

    for b in range(OWN):
        sendt[b] = feat[:, pl.ds(BLK * place_of[b], BLK)].T
    shift = lax.rem(BLK - z * rows, BLK)
    fown[...] = jnp.concatenate(
        [
            pltpu.roll(feat[:, pl.ds(BLK * place_of[b], BLK)].astype(jnp.float32), shift, 1)[:, :rows]
            for b in range(OWN)
        ]
        + [jnp.zeros((BLK, BLK - OWN * rows), jnp.float32)],
        axis=1,
    )
    own_present = jnp.concatenate(
        [pltpu.roll(boxes[b], shift, 1)[3:4, :rows] for b in range(OWN)]
        + [jnp.zeros((1, BLK - OWN * rows), jnp.float32)],
        axis=1,
    )
    mix_copy.wait()
    for n in range(4):
        mixt[:, pl.ds(BLK * n, BLK)] = mixv[n].T
    remote(wst.at[pl.ds(0, nc - 1)], w_sem).wait_recv()
    for k in range(NR):
        whole = jnp.concatenate([wst[s, :, cz * k : cz * (k + 1)] for s in range(nc)], axis=1)
        for l in range(3):
            wb[l, k] = jnp.broadcast_to(whole[l : l + 1, :], (8, BLK))
        if k == 0:
            readcol[...] = jnp.broadcast_to(whole[3:4, :], (BLK, BLK)).T
    remote(halo, halo_sem).wait_recv()
    for side in range(2):
        bit = meta_in[side, 0][5 - side : 6 - side, :] > 0.5
        early = halo[side, :, 0:BLK].astype(jnp.float32)
        late = halo[side, :, BLK : 2 * BLK].astype(jnp.float32)
        sendt[OWN + 2 * side] = jnp.where(bit, late, early).astype(jnp.bfloat16).T
        sendt[OWN + 2 * side + 1] = jnp.where(bit, early, late).astype(jnp.bfloat16).T

    def message(p):
        q0 = pairs[0, 1, slot_tile[2 * p]]
        q1 = pairs[0, 1, slot_tile[2 * p + 1]]
        both = jnp.concatenate([sendt[q0], sendt[q1]], axis=0)
        kept = keep[p].astype(jnp.float32)
        part = jnp.dot(kt[p], both, preferred_element_type=jnp.float32)
        for m in range(NM):
            acc = 0.0 if p == 0 else run[p - 1, pl.ds(m * rows, rows), :] * kept
            for k in range(NR):
                w = wb[degree[m], k]
                at = (m * NR + k) * rows
                acc = acc + jnp.concatenate([w] * (rows // 8), axis=0) * part[at : at + rows, :]
            run[p, pl.ds(m * rows, rows), :] = acc

    for p in range(PAIRS):
        message(p)

    basis = []
    for b in range(OWN):
        slot = last_slot[b]
        den = [run[slot, pl.ds(m * rows, rows), :] for m in range(NM)]
        vec = den[1] * den[1] + den[2] * den[2] + den[3] * den[3]
        ten = sum(den[m] * den[m] for m in range(5, NM)) + den[4] * den[4]
        basis.append(jnp.concatenate([den[0], den[0] * den[0], vec, ten], axis=1))
    basis = jnp.concatenate(
        basis + [jnp.zeros((BLK - OWN * rows, 4 * BLK), jnp.float32)], axis=0
    ).astype(jnp.bfloat16)
    mixed = lax.dot_general(
        mixt[...], basis, (((1,), (1,)), ((), ())), preferred_element_type=jnp.float32
    )
    hidden = fown[...] + mixed / (1.0 + jnp.exp(-mixed))
    energy = jnp.sum(readcol[...] * hidden, axis=0, keepdims=True)
    square = jnp.sum(energy * energy * own_present, axis=1, keepdims=True)
    est[z] = jnp.where(lane < OWN * rows, energy, jnp.broadcast_to(square, (1, BLK)))

    for d in far_first:
        remote(est.at[z], e_sem, chan_peer(d)).start()
    ust_send[...] = (hidden * own_present).astype(jnp.bfloat16)
    ust[z] = ust_send[own_rows, :]
    for d in far_first:
        part = pl.ds(pl.multiple_of(wrap(z + d, nc) * cz, cz), cz)
        remote(ust_send.at[part], u_sem, chan_peer(d), ust.at[z]).start()
    remote(est.at[pl.ds(0, nc - 1)], e_sem).wait_recv()
    group = est[0]
    for s in range(1, nc):
        group = group + est[s]
    atoms = zero_row
    for b in range(OWN):
        atoms = atoms + counts[b].astype(jnp.float32)
    plane[g] = jnp.where(lane < OWN * rows, atoms, group)

    if ny > 1:
        pl.semaphore_wait(ready, ny - 1)
    for n in range(na - 1):
        d = (n + (3 * na) // 8) % (na - 1) + 1
        remote(plane.at[g], plane_sem, (wrap(g + d, na), z)).start()
    energies = []
    for b in range(OWN):
        line = jnp.concatenate(
            [est[s, 0:1, rows * b : rows * (b + 1)] for s in range(nc)], axis=1
        )
        energies.append(line * boxes[b][3:4, :])
    energies = jnp.concatenate(energies, axis=0)
    remote(ust.at[pl.ds(0, nc - 1)], u_sem).wait_recv()
    for b in range(OWN):
        upd_out[:, pl.ds(BLK * b, BLK)] = jnp.concatenate(
            [ust[s].astype(jnp.float32)[:, rows * b : rows * (b + 1)] for s in range(nc)], axis=1
        ).astype(jnp.bfloat16)
    others = remote(plane.at[pl.ds(0, na - 1)], plane_sem)
    others.wait_recv()
    whole = jnp.sum(plane[:, 0, :], axis=0, keepdims=True)
    scale = jnp.sqrt(1.0 + whole[:, BLK - 1 : BLK] / whole[:, 0:1])
    energy_out[...] = energies / scale
    scale_out[...] = jnp.broadcast_to(scale, (1, BLK))

    remote(kt.at[0, pl.ds(0, 32 * nc * 2)], halo_sem).wait_send()
    remote(wst.at[pl.ds(0, nc - 1)], w_sem).wait_send()
    remote(est.at[pl.ds(0, nc - 1)], e_sem).wait_send()
    remote(ust.at[pl.ds(0, nc - 1)], u_sem).wait_send()
    others.wait_send()


def scoped(na, nc, *refs):
    pl.run_scoped(lambda sem: kernel(na, nc, *refs, sem), pltpu.SemaphoreType.DMA((9,)))


def settle(*refs):
    pl.run_scoped(lambda sems: hand_over(*refs, sems), pltpu.SemaphoreType.DMA((3,)))


def hand_over(updated, energies, scale, updated_out, energies_out, scale_out, sems):
    copies = [
        pltpu.make_async_copy(src, dst, sems.at[n])
        for n, (src, dst) in enumerate(
            ((updated, updated_out), (energies, energies_out), (scale, scale_out))
        )
    ]
    for c in copies:
        c.start()
    for c in copies:
        c.wait()


def per_device(
    na, nc, features, positions, block_counts, radial_w, mix_w, read_w, ghost_lists, tile_pairs, tile_count
):
    cz, width = features.shape
    rows = BLK // nc
    tiles = tile_pairs.shape[1]
    radial_w = radial_w.transpose(1, 0, 2)
    tile_pairs = tile_pairs.transpose(0, 2, 1)
    f32, bf16, i32 = jnp.float32, jnp.bfloat16, jnp.int32
    vm, sm, dma = pltpu.VMEM, pltpu.SMEM, pltpu.SemaphoreType.DMA
    hbm = pl.BlockSpec(memory_space=pltpu.HBM)
    vmem = pl.BlockSpec(memory_space=pltpu.VMEM)
    features, positions, block_counts, radial_w, mix_w, read_w, ghost_lists, tile_pairs = (
        pltpu.with_memory_space_constraint(v, pltpu.HBM)
        for v in (features, positions, block_counts, radial_w, mix_w, read_w, ghost_lists, tile_pairs)
    )
    updated, energies, scale = pl.pallas_call(
        functools.partial(scoped, na, nc),
        out_shape=(
            jax.ShapeDtypeStruct((cz, width), bf16),
            jax.ShapeDtypeStruct((OWN, BLK), f32),
            jax.ShapeDtypeStruct((1, BLK), f32),
        ),
        in_specs=[hbm] * 9,
        out_specs=(vmem, vmem, vmem),
        scratch_shapes=[
            vm((BLK, width), bf16),
            vm((2, BLK, 2 * BLK), bf16),
            vm((3, width), f32),
            vm((4, BLK, BLK), bf16),
            vm((BLK, 4 * BLK), bf16),
            vm((3, NR, cz), f32),
            vm((cz,), f32),
            vm((nc, 4, BLK), f32),
            vm((3, NR, 8, BLK), f32),
            vm((BLK, BLK), f32),
            vm((2, 2, 8, BLK), f32),
            vm((2, 2, 8, BLK), f32),
            vm((2 * OWN, 8, BLK), f32),
            vm((BLK, BLK), f32),
            vm((OWN, 3, rows, BLK), f32),
            vm((2 * OWN, BLK, BLK), bf16),
            vm((PAIRS, NM * NR * rows, 2 * BLK), bf16),
            vm((PAIRS, NM * rows, BLK), f32),
            vm((BLK, BLK), f32),
            vm((BLK, BLK), bf16),
            vm((nc, cz, BLK), bf16),
            vm((nc, 1, BLK), f32),
            vm((na, 1, BLK), f32),
            sm((OWN,), i32),
            sm((1, 2, 2), i32),
            sm((1, 2, tiles), i32),
            sm((1,), i32),
            sm((tiles,), i32),
            sm((2 * PAIRS,), i32),
            sm((2 * PAIRS,), i32),
            sm((PAIRS,), i32),
            sm((OWN,), i32),
            dma((5,)),
            dma((2,)),
            dma((1,)),
            dma((1,)),
            dma((2,)),
            dma((2,)),
            dma((2,)),
            pltpu.SemaphoreType.REGULAR,
        ],
        compiler_params=pltpu.CompilerParams(
            collective_id=0, has_side_effects=True, vmem_limit_bytes=48 * 1024 * 1024
        ),
        name="message_layer",
    )(features, positions, block_counts, radial_w, mix_w, read_w, ghost_lists, tile_pairs, tile_count)
    updated, energies, scale = pl.pallas_call(
        settle,
        out_shape=(
            jax.ShapeDtypeStruct((cz, width), bf16),
            jax.ShapeDtypeStruct((OWN, BLK), f32),
            jax.ShapeDtypeStruct((1, BLK), f32),
        ),
        in_specs=[pl.BlockSpec(memory_space=pl.ANY)] * 3,
        out_specs=(hbm, hbm, hbm),
        compiler_params=pltpu.CompilerParams(vmem_limit_bytes=1024 * 1024),
        name="settle",
    )(updated, energies, scale)
    return updated, energies.reshape(width), scale[0, 0]


def solution(mesh):
    in_specs = (
        P("chan", "atoms"),
        P(None, "atoms"),
        P("atoms"),
        P(None, None, "chan"),
        P(),
        P("chan"),
        P("atoms", None, None),
        P("atoms", None, None),
        P("atoms"),
    )
    out_specs = (P("chan", "atoms"), P("atoms"), P())
    step = functools.partial(per_device, mesh.shape["atoms"], mesh.shape["chan"])
    return jax.shard_map(step, mesh=mesh, in_specs=in_specs, out_specs=out_specs, check_vma=False)
```
